128 devices in a mesh: row: 2 (over z_lo), col: 64 (over y, x, z_hi, core).
Axes of the slice: x: 4, y: 4, z: 4 (z_hi: 2, z_lo: 2; z = z_hi * 2 + z_lo), core: 2. Of those that a mesh axis runs over, the one named last changes fastest.
Arguments:
- tokens: bfloat16 [512, 4608], P('col', 'row'), may hold values from -6 to 6
- pre_gain: float32 [2, 4608], P(None, 'row'), may hold values from -0.6 to 0.6
- post_gain: float32 [2, 4608], P(None, 'row'), may hold values from -0.6 to 0.6
- gate_weight: bfloat16 [2, 4608, 36864], P(None, ('row', 'col')), may hold values from -0.09375 to 0.09375
- up_weight: bfloat16 [2, 4608, 36864], P(None, ('row', 'col')), may hold values from -0.09375 to 0.09375
- down_weight: bfloat16 [2, 36864, 4608], P(None, ('row', 'col')), may hold values from -0.13541667 to 0.13541667
Outputs:
- stream: bfloat16 [512, 4608], P('col', 'row')
The draws below stay inside these ranges and needn't reach their ends.
All inputs are finite; a program needn't handle non-finite values.
Results may differ from the reference program's by a relative error of at most 0.019.
Values may be sent and summed in bfloat16 or wider, within the bound.
No kernel may reach another device: no remote copies, remote signals or barrier semaphores. Data moves between devices by JAX's collectives and lax.ppermute only.
A program may use at most 128 MiB of HBM per device.

```python
import math
import jax
import jax.numpy as jnp
from jax import lax

D = 4608
FF = 36864
LAYERS = 2
TOKENS = 512


def draw_down_weight(key, part):
    key_main = jax.random.fold_in(key, 11)
    key_rough = jax.random.fold_in(key, 12)
    entries = jax.random.truncated_normal(key_main, -6.0, 6.0, (LAYERS, FF, D), jnp.float32)
    low_end = 0.5
    high_end = 2.0
    ramp = jnp.linspace(math.log(low_end), math.log(high_end), D, dtype=jnp.float32)
    rough = jax.random.uniform(key_rough, (LAYERS, 1, D), jnp.float32, math.log(0.7), math.log(1.4))
    scales = jnp.exp(ramp[None, None, :] + rough)
    return (entries * scales * FF ** (-0.5)).astype(jnp.bfloat16)


def block_levels(own_key, shape, shards, least, top_value):
    loudness = 1.0
    for axis_at, blocks in shards:
        draws = jax.random.uniform(jax.random.fold_in(jax.random.fold_in(own_key, 6), axis_at), (blocks,), jnp.float32, least / len(shards), top_value / len(shards))
        loudness = loudness * jnp.repeat(jnp.exp(draws), shape[axis_at] // blocks).reshape((-1,) + (1,) * (len(shape) - 1 - axis_at))
    return loudness


def bell_draw(stream_key, extent, scale, most, pieces=(), held_as=jnp.bfloat16):
    drawn = jax.random.normal(stream_key, extent, jnp.float32) * scale
    if len(pieces) > 0:
        drawn = block_levels(stream_key, extent, pieces, -0.22, 0.18) * drawn
    return jnp.clip(drawn, min=-most, max=most).astype(held_as)


def setup_inputs(seed: int = 0) -> dict:
    seeds = jax.random.split(jax.random.key(seed), 7)
    return {
        "tokens": bell_draw(seeds[0], (TOKENS, D), 1.0, 6.0, ((0, 64), (1, 2))),
        "pre_gain": jnp.clip(jax.random.uniform(seeds[1], (LAYERS, D), jnp.float32, -0.6, 0.6) * block_levels(seeds[1], (LAYERS, D), ((1, 2),), -0.4, 0.0), -0.6, 0.6),
        "post_gain": jnp.clip(jax.random.uniform(seeds[2], (LAYERS, D), jnp.float32, -0.6, 0.6) * block_levels(seeds[2], (LAYERS, D), ((1, 2),), -0.4, 0.0), -0.6, 0.6),
        "gate_weight": bell_draw(seeds[3], (LAYERS, D, FF), D ** -0.5, 0.09375, ((1, 128),)),
        "up_weight": bell_draw(seeds[4], (LAYERS, D, FF), D ** -0.5, 0.09375, ((1, 128),)),
        "down_weight": draw_down_weight(jax.random.fold_in(seeds[6], 71), 0),
    }


norm_eps = 1e-06

def reference(tokens, pre_gain, post_gain, gate_weight, up_weight, down_weight):
    current = tokens
    for layer_index in range(LAYERS):
        values = current.astype(jnp.float32)
        mean_sq = lax.optimization_barrier(jnp.mean(values * values, axis=1, keepdims=True))
        normed = (values * lax.rsqrt(mean_sq + norm_eps) * (1.0 + pre_gain[layer_index])[None, :]).astype(jnp.bfloat16)
        gate = jnp.dot(normed, gate_weight[layer_index], preferred_element_type=jnp.float32)
        up_proj = jnp.dot(normed, up_weight[layer_index], preferred_element_type=jnp.float32)
        hidden = (jax.nn.gelu(gate, approximate=True) * up_proj).astype(jnp.bfloat16)
        branch = jnp.dot(hidden, down_weight[layer_index], preferred_element_type=jnp.float32)
        branch_sq = lax.optimization_barrier(jnp.mean(branch * branch, axis=1, keepdims=True))
        post = branch * lax.rsqrt(branch_sq + norm_eps) * (1.0 + post_gain[layer_index])[None, :]
        current = (values + post).astype(jnp.bfloat16)
    return current
```

```python
import jax
import jax.numpy as jnp
from jax import lax
from jax.experimental import pallas as pl
from jax.experimental.pallas import tpu as pltpu
from jax.sharding import Mesh
from jax.sharding import PartitionSpec as P

COL = ("col_0", "col_1", "col_2", "core")
ROW_COL = ("row", *COL)
CHIP = ("row", "col_0", "col_1", "col_2")

norm_eps = 1e-06


def pack_kernel(gate_ref, up_ref, out_ref):
    layers, rows, width = gate_ref.shape
    whole = rows // 8 * 8
    rest = rows - whole
    half = width // 2
    aligned = half // 128 * 128
    odd = half - aligned
    for side in range(2):
        first = 0 if side == 0 else width - aligned
        extra = aligned if side == 0 else half
        for layer in range(layers):
            places = (
                (slice(0, whole), slice(layer * whole, (layer + 1) * whole)),
                (
                    slice(whole, rows),
                    slice(layers * whole + layer * rest, layers * whole + (layer + 1) * rest),
                ),
            )
            for taken, put in places:
                out_ref[side, put, 0:aligned] = gate_ref[layer, taken, first : first + aligned]
                out_ref[side, put, aligned : 2 * aligned] = up_ref[
                    layer, taken, first : first + aligned
                ]
                out_ref[side, put, 2 * aligned : 2 * aligned + odd] = gate_ref[
                    layer, taken, extra : extra + odd
                ]
                out_ref[side, put, 2 * aligned + odd : width] = up_ref[
                    layer, taken, extra : extra + odd
                ]


def packed(gate_weight, up_weight, chips):
    layers, rows, hidden = gate_weight.shape
    width = hidden // chips * 2
    taken = pl.BlockSpec((layers, rows, width), lambda i: (0, 0, i))
    return pl.pallas_call(
        pack_kernel,
        grid=(chips // 2,),
        in_specs=[taken, taken],
        out_specs=pl.BlockSpec((2, layers * rows, width), lambda i: (i, 0, 0)),
        out_shape=jax.ShapeDtypeStruct((chips, layers * rows, width), gate_weight.dtype),
        name="pack",
    )(gate_weight, up_weight)


def gate_up_kernel(main_ref, rest_ref, weight_ref, weight_rest_ref, out_ref, total_ref):
    step = pl.program_id(0)
    width = weight_ref.shape[2]
    part = jnp.dot(
        main_ref[...], weight_ref[...].reshape(-1, width), preferred_element_type=jnp.float32
    )
    part += jnp.dot(
        rest_ref[...], weight_rest_ref[...].reshape(-1, width), preferred_element_type=jnp.float32
    )

    @pl.when(step == 0)
    def _():
        total_ref[...] = part

    @pl.when(step > 0)
    def _():
        total_ref[...] += part

    @pl.when(step == pl.num_programs(0) - 1)
    def _():
        out_ref[...] = total_ref[...].astype(out_ref.dtype)


def gate_up(normed, tiles, layer, layers):
    tokens = normed.shape[0]
    chips, rows, width = tiles.shape
    whole = rows // layers // 8 * 8
    rest = rows - layers * whole
    group = 128 // rest
    steps = chips // group
    return pl.pallas_call(
        gate_up_kernel,
        grid=(steps,),
        in_specs=[
            pl.BlockSpec((tokens, group * whole), lambda i: (0, i)),
            pl.BlockSpec((tokens, group * rest), lambda i: (0, chips * whole // 128 + i)),
            pl.BlockSpec((group, whole, width), lambda i: (i, layer, 0)),
            pl.BlockSpec((group, rest, width), lambda i: (i, layers * whole // rest, 0)),
        ],
        out_specs=pl.BlockSpec((tokens, width), lambda i: (0, 0)),
        out_shape=jax.ShapeDtypeStruct((tokens, width), jnp.bfloat16),
        scratch_shapes=[pltpu.VMEM((tokens, width), jnp.float32)],
        name="gate_up",
    )(normed, normed, tiles, tiles)


def copies_of(value, axes):
    return jnp.broadcast_to(value, (lax.axis_size(axes), *value.shape))


def exchanged(blocks, axes):
    return lax.all_to_all(blocks, axes, split_axis=0, concat_axis=0, tiled=True)


def slabs(normed, layer, layers, chips, cores):
    count, model_width = normed.shape
    rows = model_width // (chips * cores)
    whole = rows // 8 * 8
    rest = rows - whole
    cut = normed.reshape(count, chips, cores, rows).transpose(2, 0, 1, 3)
    main = cut[..., :whole].reshape(cores, count, chips * whole)
    tail = jnp.pad(
        cut[..., whole:], ((0, 0), (0, 0), (0, 0), (layer * rest, (layers - 1 - layer) * rest))
    ).reshape(cores, count, chips * rest * layers)
    return jnp.concatenate((main, tail), axis=2)


def on_device(tokens, pre_gain, post_gain, gate_weight, up_weight, down_weight):
    layers = gate_weight.shape[0]
    chips = lax.axis_size(CHIP)
    cores = lax.axis_size("core")
    model_width = tokens.shape[1] * lax.axis_size("row")
    core = lax.axis_index("core")
    side = lax.axis_index("col_2")

    current = lax.all_to_all(tokens, "row", split_axis=0, concat_axis=1, tiled=True)
    gains = exchanged(copies_of(jnp.concatenate((pre_gain, post_gain), axis=0), "row"), "row")
    gains = 1.0 + jnp.concatenate((gains[0], gains[1]), axis=1)
    count = current.shape[0]

    tiles = exchanged(packed(gate_weight, up_weight, chips), CHIP)
    other_down = lax.ppermute(down_weight, "core", [(0, 1), (1, 0)])

    for layer in range(layers):
        values = current.astype(jnp.float32)
        scale_pre = lax.rsqrt(jnp.mean(values * values, axis=1, keepdims=True) + norm_eps)
        normed = (values * scale_pre * gains[layer][None, :]).astype(jnp.bfloat16)
        cut = exchanged(slabs(normed, layer, layers, chips, cores), "core")
        cut = cut.reshape(cores * count, -1)
        everything = exchanged(copies_of(cut, CHIP), CHIP).reshape(-1, cut.shape[1])
        partial = gate_up(everything, tiles, layer, layers)
        width = partial.shape[1]
        partial = partial.reshape(chips, cores, count, width).transpose(1, 0, 2, 3)
        both = exchanged(partial.reshape(cores, chips * count, width), "core")
        summed = both[0].astype(jnp.float32) + both[1].astype(jnp.float32)
        half = width // 2
        aligned = half // 128 * 128
        gate = jnp.concatenate(
            (summed[:, :aligned], summed[:, 2 * aligned : half + aligned]), axis=1
        )
        up_proj = jnp.concatenate(
            (summed[:, aligned : 2 * aligned], summed[:, half + aligned :]), axis=1
        )
        hidden = (jax.nn.gelu(gate, approximate=True) * up_proj).astype(jnp.bfloat16)
        turned = jnp.concatenate((hidden[:, aligned:], hidden[:, :aligned]), axis=1)
        hidden = jnp.where(side == 0, hidden, turned)
        stored = down_weight.shape[1]
        low, high = hidden[:, :stored], hidden[:, stored:]
        own = jnp.where(core == 0, low, high)
        other = jnp.where(core == 0, high, low)
        branch = jnp.dot(own, down_weight[layer], preferred_element_type=jnp.float32)
        branch += jnp.dot(other, other_down[layer], preferred_element_type=jnp.float32)
        arrived = exchanged(branch.astype(jnp.bfloat16).reshape(chips, count, -1), CHIP)
        branch = jnp.sum(arrived.astype(jnp.float32), axis=0)
        scale_post = lax.rsqrt(jnp.mean(branch * branch, axis=1, keepdims=True) + norm_eps)
        post = branch * scale_post * gains[layers + layer][None, :]
        current = (values + post).astype(jnp.bfloat16)
    return lax.all_to_all(current, "row", split_axis=1, concat_axis=0, tiled=True)


def solution(mesh):
    split = Mesh(
        mesh.devices.reshape(mesh.shape["row"], 4, 4, 2, 2),
        ROW_COL,
    )
    in_specs = (
        P(COL, "row"),
        P(None, "row"),
        P(None, "row"),
        P(None, ROW_COL, None),
        P(None, ROW_COL, None),
        P(None, ROW_COL, None),
    )
    out_specs = P(COL, "row")
    return jax.shard_map(
        on_device, mesh=split, in_specs=in_specs, out_specs=out_specs, check_vma=False
    )
```

```python
import functools

import jax
import jax.numpy as jnp
from jax import lax
from jax.experimental import pallas as pl
from jax.experimental.pallas import tpu as pltpu
from jax.sharding import Mesh
from jax.sharding import PartitionSpec as P

COL = ("col_0", "col_1", "col_2", "core")
ROW_COL = ("row", *COL)
CHIP = ("row", "col_0", "col_1", "col_2")

SWAP = [(0, 1), (1, 0)]

norm_eps = 1e-06


def pack_kernel(gate_ref, up_ref, first_ref, later_ref):
    rows, layers, lanes = gate_ref.shape
    pairs = first_ref.shape[0] // 2
    width = lanes // pairs
    whole = rows // 8 * 8
    rest = rows - whole
    half = width // 2
    aligned = half // 128 * 128
    odd = half - aligned
    for pair in range(pairs):
        for index, ref in enumerate((gate_ref, up_ref)):
            block = jnp.swapaxes(ref[:, :, pair * width : (pair + 1) * width], 0, 1)
            for side in range(2):
                first = 0 if side == 0 else width - aligned
                extra = aligned if side == 0 else half
                main = slice(index * aligned, (index + 1) * aligned)
                tail = slice(2 * aligned + index * odd, 2 * aligned + (index + 1) * odd)
                place = 2 * pair + side
                for layer in range(layers):
                    out_ref = first_ref if layer == 0 else later_ref
                    start = 0 if layer == 0 else (layer - 1) * whole
                    put = slice(start, start + whole)
                    out_ref[place, put, main] = block[layer, :whole, first : first + aligned]
                    out_ref[place, put, tail] = block[layer, :whole, extra : extra + odd]
                    put = slice(whole + layer * rest, whole + (layer + 1) * rest)
                    first_ref[place, put, main] = block[layer, whole:, first : first + aligned]
                    first_ref[place, put, tail] = block[layer, whole:, extra : extra + odd]


def packed(gate_weight, up_weight, chips):
    layers, rows, hidden = gate_weight.shape
    width = hidden // chips * 2
    whole = rows // 8 * 8
    pairs = 4
    taken = pl.BlockSpec((rows, layers, pairs * width), lambda i: (0, 0, i))
    lengths = (whole + layers * (rows - whole), (layers - 1) * whole)
    return pl.pallas_call(
        pack_kernel,
        grid=(chips // 2 // pairs,),
        in_specs=[taken, taken],
        out_specs=[pl.BlockSpec((2 * pairs, n, width), lambda i: (i, 0, 0)) for n in lengths],
        out_shape=[jax.ShapeDtypeStruct((chips, n, width), gate_weight.dtype) for n in lengths],
        compiler_params=pltpu.CompilerParams(vmem_limit_bytes=48 * 2**20),
        name="pack",
    )(jnp.swapaxes(gate_weight, 0, 1), jnp.swapaxes(up_weight, 0, 1))


def gate_up_kernel(
    layer, core_ref, normed_ref, weight_ref, rest_ref, own_ref, other_ref, spread_ref
):
    tokens = normed_ref.shape[0]
    chips, whole, width = weight_ref.shape
    rest = rest_ref.shape[1]
    own = own_ref.shape[0]
    cores = tokens // own
    count = own // chips
    narrow = normed_ref.shape[1] - chips * whole

    @pl.when(pl.program_id(0) == 0)
    def _():
        part = narrow // chips
        taken = lax.broadcasted_iota(jnp.int32, (narrow, chips * rest), 0)
        put = lax.broadcasted_iota(jnp.int32, (narrow, chips * rest), 1)
        place = taken // part * rest + layer * part + taken % part
        spread_ref[...] = jnp.dot(
            normed_ref[:, chips * whole :],
            (place == put).astype(jnp.float32).astype(jnp.bfloat16),
            preferred_element_type=jnp.float32,
        ).astype(jnp.bfloat16)

    part = jnp.dot(
        normed_ref[:, : chips * whole],
        weight_ref[...].reshape(chips * whole, width),
        preferred_element_type=jnp.float32,
    )
    part += jnp.dot(
        spread_ref[...],
        rest_ref[...].reshape(chips * rest, width),
        preferred_element_type=jnp.float32,
    )
    put = lax.broadcasted_iota(jnp.int32, (tokens, tokens), 0)
    taken = lax.broadcasted_iota(jnp.int32, (tokens, tokens), 1)
    owner = (put // own + core_ref[0]) % cores
    place = put % own // count * (cores * count) + owner * count + put % count
    ordered = jnp.dot(
        (place == taken).astype(jnp.float32).astype(jnp.bfloat16),
        part.astype(jnp.bfloat16),
        preferred_element_type=jnp.float32,
    ).astype(own_ref.dtype)
    own_ref[...] = ordered[:own]
    other_ref[...] = ordered[own:]


def gate_up(normed, weights, rests, layer, core, cores):
    tokens, depth = normed.shape
    chips, _, width = weights.shape
    layers = 2
    rows = depth // chips
    whole = rows // 8 * 8
    rest = layers * (rows - whole)
    step = 384
    own = tokens // cores
    return pl.pallas_call(
        functools.partial(gate_up_kernel, layer),
        grid=(width // step,),
        in_specs=[
            pl.BlockSpec(memory_space=pltpu.SMEM),
            pl.BlockSpec((tokens, depth), lambda i: (0, 0)),
            pl.BlockSpec((chips, whole, step), lambda i: (0, 0, i)),
            pl.BlockSpec((chips, rest, step), lambda i: (0, whole // rest, i)),
        ],
        out_specs=[pl.BlockSpec((own, step), lambda i: (0, i))] * 2,
        out_shape=[jax.ShapeDtypeStruct((own, width), jnp.bfloat16)] * 2,
        scratch_shapes=[pltpu.VMEM((tokens, chips * rest), jnp.bfloat16)],
        compiler_params=pltpu.CompilerParams(vmem_limit_bytes=40 * 2**20),
        name="gate_up",
    )(core.reshape(1), normed, weights, rests)


def copies_of(value, axes):
    return jnp.broadcast_to(value, (lax.axis_size(axes), *value.shape))


def exchanged(blocks, axes):
    return lax.all_to_all(blocks, axes, split_axis=0, concat_axis=0, tiled=True)


def slabs(normed, chips, cores):
    count, model_width = normed.shape
    rows = model_width // (chips * cores)
    whole = rows // 8 * 8
    cut = normed.reshape(count, chips, cores, rows).transpose(2, 0, 1, 3)
    main = cut[..., :whole].reshape(cores, count, chips * whole)
    tail = cut[..., whole:].reshape(cores, count, chips * (rows - whole))
    return jnp.concatenate((main, tail), axis=2)


def on_device(tokens, pre_gain, post_gain, gate_weight, up_weight, down_weight):
    layers = gate_weight.shape[0]
    chips = lax.axis_size(CHIP)
    cores = lax.axis_size("core")
    core = lax.axis_index("core")
    side = lax.axis_index("col_2")

    count = tokens.shape[0] // lax.axis_size("row")
    gains = copies_of(jnp.concatenate((pre_gain, post_gain), axis=0), "row")
    mixed = tokens.reshape(-1, count, tokens.shape[1]).astype(jnp.float32)
    mixed = exchanged(jnp.concatenate((mixed, gains), axis=1), "row")
    mixed = jnp.concatenate((mixed[0], mixed[1]), axis=1)
    current = mixed[:count].astype(jnp.bfloat16)
    gains = 1.0 + mixed[count:]

    other_down = lax.ppermute(down_weight, "core", SWAP)
    first, later = packed(gate_weight, up_weight, chips)
    first, other_down = lax.optimization_barrier((first, other_down))
    first = exchanged(first, CHIP)
    later = exchanged(later, CHIP)

    for layer in range(layers):
        values = current.astype(jnp.float32)
        scale_pre = lax.rsqrt(jnp.mean(values * values, axis=1, keepdims=True) + norm_eps)
        normed = (values * scale_pre * gains[layer][None, :]).astype(jnp.bfloat16)
        cut = exchanged(slabs(normed, chips, cores), "core")
        cut = cut.reshape(cores * count, -1)
        everything = exchanged(copies_of(cut, CHIP), CHIP).reshape(-1, cut.shape[1])
        weights = first if layer == 0 else later
        mine, theirs = gate_up(everything, weights, first, layer, core, cores)
        width = mine.shape[1]
        arrived = lax.ppermute(theirs, "core", SWAP)
        summed = mine.astype(jnp.float32) + arrived.astype(jnp.float32)
        half = width // 2
        aligned = half // 128 * 128
        gate = jnp.concatenate(
            (summed[:, :aligned], summed[:, 2 * aligned : half + aligned]), axis=1
        )
        up_proj = jnp.concatenate(
            (summed[:, aligned : 2 * aligned], summed[:, half + aligned :]), axis=1
        )
        hidden = (jax.nn.gelu(gate, approximate=True) * up_proj).astype(jnp.bfloat16)
        turned = jnp.concatenate((hidden[:, aligned:], hidden[:, :aligned]), axis=1)
        hidden = jnp.where(side == 0, hidden, turned)
        stored = down_weight.shape[1]
        low, high = hidden[:, :stored], hidden[:, stored:]
        own = jnp.where(core == 0, low, high)
        other = jnp.where(core == 0, high, low)
        branch = jnp.dot(own, down_weight[layer], preferred_element_type=jnp.float32)
        branch += jnp.dot(other, other_down[layer], preferred_element_type=jnp.float32)
        sent = branch.astype(jnp.bfloat16)
        if layer == 0:
            sent, later = lax.optimization_barrier((sent, later))
        arrived = exchanged(sent.reshape(chips, count, -1), CHIP)
        branch = jnp.sum(arrived.astype(jnp.float32), axis=0)
        scale_post = lax.rsqrt(jnp.mean(branch * branch, axis=1, keepdims=True) + norm_eps)
        post = branch * scale_post * gains[layers + layer][None, :]
        current = (values + post).astype(jnp.bfloat16)
    return lax.all_to_all(current, "row", split_axis=1, concat_axis=0, tiled=True)


def solution(mesh):
    split = Mesh(
        mesh.devices.reshape(mesh.shape["row"], 4, 4, 2, 2),
        ROW_COL,
    )
    in_specs = (
        P(COL, "row"),
        P(None, "row"),
        P(None, "row"),
        P(None, ROW_COL, None),
        P(None, ROW_COL, None),
        P(None, ROW_COL, None),
    )
    out_specs = P(COL, "row")

    return jax.shard_map(
        on_device, mesh=split, in_specs=in_specs, out_specs=out_specs, check_vma=False
    )
```

```python
import functools

import jax
import jax.numpy as jnp
from jax import lax
from jax.experimental import pallas as pl
from jax.experimental.pallas import tpu as pltpu
from jax.sharding import Mesh
from jax.sharding import PartitionSpec as P

COL = ("col_0", "col_1", "col_2", "core")
ROW_COL = ("row", *COL)
CHIP = ("row", "col_0", "col_1", "col_2")

SWAP = [(0, 1), (1, 0)]

norm_eps = 1e-06


def pack_kernel(gate_ref, up_ref, first_ref, later_ref):
    rows, layers, lanes = gate_ref.shape
    pairs = first_ref.shape[0] // 2
    width = lanes // pairs
    whole = rows // 8 * 8
    rest = rows - whole
    half = width // 2
    aligned = half // 128 * 128
    odd = half - aligned
    for pair in range(pairs):
        for index, ref in enumerate((gate_ref, up_ref)):
            block = jnp.swapaxes(ref[:, :, pair * width : (pair + 1) * width], 0, 1)
            for side in range(2):
                first = 0 if side == 0 else width - aligned
                extra = aligned if side == 0 else half
                main = slice(index * aligned, (index + 1) * aligned)
                tail = slice(2 * aligned + index * odd, 2 * aligned + (index + 1) * odd)
                place = 2 * pair + side
                for layer in range(layers):
                    out_ref = first_ref if layer == 0 else later_ref
                    start = 0 if layer == 0 else (layer - 1) * whole
                    put = slice(start, start + whole)
                    out_ref[place, put, main] = block[layer, :whole, first : first + aligned]
                    out_ref[place, put, tail] = block[layer, :whole, extra : extra + odd]
                    put = slice(whole + layer * rest, whole + (layer + 1) * rest)
                    first_ref[place, put, main] = block[layer, whole:, first : first + aligned]
                    first_ref[place, put, tail] = block[layer, whole:, extra : extra + odd]


def packed(gate_weight, up_weight, chips):
    layers, rows, hidden = gate_weight.shape
    width = hidden // chips * 2
    whole = rows // 8 * 8
    pairs = 4
    taken = pl.BlockSpec((rows, layers, pairs * width), lambda i: (0, 0, i))
    lengths = (whole + layers * (rows - whole), (layers - 1) * whole)
    return pl.pallas_call(
        pack_kernel,
        grid=(chips // 2 // pairs,),
        in_specs=[taken, taken],
        out_specs=[pl.BlockSpec((2 * pairs, n, width), lambda i: (i, 0, 0)) for n in lengths],
        out_shape=[jax.ShapeDtypeStruct((chips, n, width), gate_weight.dtype) for n in lengths],
        compiler_params=pltpu.CompilerParams(vmem_limit_bytes=59 * 2**20),
        name="pack",
    )(jnp.swapaxes(gate_weight, 0, 1), jnp.swapaxes(up_weight, 0, 1))


def bits(length):
    return length.bit_length() - 1


def one_hot(place, taken):
    return (place == taken).astype(jnp.float32).astype(jnp.bfloat16)


def gate_up_kernel(
    layer, core_ref, normed_ref, weight_ref, rest_ref, own_ref, other_ref, spread_ref, order_ref
):
    tokens = normed_ref.shape[0]
    chips, whole, width = weight_ref.shape
    rest = rest_ref.shape[1]
    own = own_ref.shape[0]
    cores = tokens // own
    count = own // chips
    narrow = normed_ref.shape[1] - chips * whole

    @pl.when(pl.program_id(0) == 0)
    def _():
        part = narrow // chips
        taken = lax.broadcasted_iota(jnp.int32, (narrow, chips * rest), 0)
        put = lax.broadcasted_iota(jnp.int32, (narrow, chips * rest), 1)
        place = ((taken >> bits(part)) << bits(rest)) + layer * part + (taken & (part - 1))
        spread_ref[...] = jnp.dot(
            normed_ref[:, chips * whole :],
            one_hot(place, put),
            preferred_element_type=jnp.float32,
        ).astype(jnp.bfloat16)
        put = lax.broadcasted_iota(jnp.int32, (tokens, tokens), 0)
        taken = lax.broadcasted_iota(jnp.int32, (tokens, tokens), 1)
        owner = ((put >> bits(own)) + core_ref[0]) & (cores - 1)
        chip = (put & (own - 1)) >> bits(count)
        place = chip * (cores * count) + owner * count + (put & (count - 1))
        order_ref[...] = one_hot(place, taken)

    part = jnp.dot(
        normed_ref[:, : chips * whole],
        weight_ref[...].reshape(chips * whole, width),
        preferred_element_type=jnp.float32,
    )
    part += jnp.dot(
        spread_ref[...],
        rest_ref[...].reshape(chips * rest, width),
        preferred_element_type=jnp.float32,
    )
    ordered = jnp.dot(
        order_ref[...], part.astype(jnp.bfloat16), preferred_element_type=jnp.float32
    ).astype(own_ref.dtype)
    own_ref[...] = ordered[:own]
    other_ref[...] = ordered[own:]


def gate_up(normed, weights, rests, layer, core, cores):
    tokens, depth = normed.shape
    chips, _, width = weights.shape
    layers = 2
    rows = depth // chips
    whole = rows // 8 * 8
    rest = layers * (rows - whole)
    step = 384
    own = tokens // cores
    return pl.pallas_call(
        functools.partial(gate_up_kernel, layer),
        grid=(width // step,),
        in_specs=[
            pl.BlockSpec(memory_space=pltpu.SMEM),
            pl.BlockSpec((tokens, depth), lambda i: (0, 0)),
            pl.BlockSpec((chips, whole, step), lambda i: (0, 0, i)),
            pl.BlockSpec((chips, rest, step), lambda i: (0, whole // rest, i)),
        ],
        out_specs=[pl.BlockSpec((own, step), lambda i: (0, i))] * 2,
        out_shape=[jax.ShapeDtypeStruct((own, width), jnp.bfloat16)] * 2,
        scratch_shapes=[
            pltpu.VMEM((tokens, chips * rest), jnp.bfloat16),
            pltpu.VMEM((tokens, tokens), jnp.bfloat16),
        ],
        compiler_params=pltpu.CompilerParams(vmem_limit_bytes=56 * 2**20),
        name="gate_up",
    )(core.reshape(1), normed, weights, rests)


def down_kernel(place_ref, mine_ref, got_ref, *refs):
    own_low_ref, own_high_ref, other_low_ref, other_high_ref, out_ref = refs[:5]
    hidden_ref, own_ref, other_ref, order_ref = refs[5:]
    rows, width = mine_ref.shape
    half = width // 2
    aligned = half // 128 * 128
    stored = own_ref.shape[1]
    chips, put_rows, step = out_ref.shape
    count = put_rows // 2

    @pl.when(pl.program_id(0) == 0)
    def _():
        summed = mine_ref[...].astype(jnp.float32) + got_ref[...].astype(jnp.float32)
        main = jax.nn.gelu(summed[:, :aligned], approximate=True)
        main = (main * summed[:, aligned : 2 * aligned]).astype(jnp.bfloat16)
        tail = jax.nn.gelu(summed[:, 2 * aligned : half + aligned], approximate=True)
        tail = (tail * summed[:, half + aligned :]).astype(jnp.bfloat16)

        @pl.when(place_ref[1] == 0)
        def _():
            hidden_ref[:, :aligned] = main
            hidden_ref[:, aligned:] = tail

        @pl.when(place_ref[1] != 0)
        def _():
            hidden_ref[:, : half - aligned] = tail
            hidden_ref[:, half - aligned :] = main

        @pl.when(place_ref[0] == 0)
        def _():
            own_ref[...] = hidden_ref[:, :stored]
            other_ref[...] = hidden_ref[:, stored:]

        @pl.when(place_ref[0] != 0)
        def _():
            own_ref[...] = hidden_ref[:, stored:]
            other_ref[...] = hidden_ref[:, :stored]

        put = lax.broadcasted_iota(jnp.int32, (2 * rows, 2 * rows), 0)
        taken = lax.broadcasted_iota(jnp.int32, (2 * rows, 2 * rows), 1)
        side = (put >> bits(count)) & 1
        place = side * rows + ((put >> bits(put_rows)) << bits(count)) + (put & (count - 1))
        order_ref[...] = one_hot(place, taken)

    sides = []
    for mine, theirs in ((own_low_ref, other_low_ref), (own_high_ref, other_high_ref)):
        part = jnp.dot(own_ref[...], mine[0], preferred_element_type=jnp.float32)
        part += jnp.dot(other_ref[...], theirs[0], preferred_element_type=jnp.float32)
        sides.append(part.astype(jnp.bfloat16))
    ordered = jnp.dot(
        order_ref[...], jnp.concatenate(sides, axis=0), preferred_element_type=jnp.float32
    )
    out_ref[...] = ordered.reshape(chips, put_rows, step).astype(out_ref.dtype)


def down(mine, got, own_down, other_down, layer, place, chips):
    rows, width = mine.shape
    _, stored, model_width = own_down.shape
    step = 384
    steps = model_width // 2 // step
    whole = pl.BlockSpec((rows, width), lambda i: (0, 0))
    low = pl.BlockSpec((1, stored, step), lambda i: (layer, 0, i))
    high = pl.BlockSpec((1, stored, step), lambda i: (layer, 0, steps + i))
    put_rows = 2 * rows // chips
    return pl.pallas_call(
        down_kernel,
        grid=(steps,),
        in_specs=[pl.BlockSpec(memory_space=pltpu.SMEM), whole, whole, low, high, low, high],
        out_specs=pl.BlockSpec((chips, put_rows, step), lambda i: (0, 0, i)),
        out_shape=jax.ShapeDtypeStruct((chips, put_rows, model_width // 2), jnp.bfloat16),
        scratch_shapes=[
            pltpu.VMEM((rows, width // 2), jnp.bfloat16),
            pltpu.VMEM((rows, stored), jnp.bfloat16),
            pltpu.VMEM((rows, stored), jnp.bfloat16),
            pltpu.VMEM((2 * rows, 2 * rows), jnp.bfloat16),
        ],
        compiler_params=pltpu.CompilerParams(vmem_limit_bytes=48 * 2**20),
        name="down",
    )(place, mine, got, own_down, own_down, other_down, other_down)


def copies_of(value, axes):
    return jnp.broadcast_to(value, (lax.axis_size(axes), *value.shape))


def exchanged(blocks, axes):
    return lax.all_to_all(blocks, axes, split_axis=0, concat_axis=0, tiled=True)


def slabs(normed, chips, cores):
    halves, count, model_half = normed.shape
    rows = model_half * halves // (chips * cores)
    whole = rows // 8 * 8
    cut = normed.reshape(halves, count, chips // halves, cores, rows).transpose(3, 1, 0, 2, 4)
    main = cut[..., :whole].reshape(cores, count, chips * whole)
    tail = cut[..., whole:].reshape(cores, count, chips * (rows - whole))
    return jnp.concatenate((main, tail), axis=2)


def scale_of(values):
    squares = jnp.sum(values * values, axis=(0, 2), keepdims=True)
    return lax.rsqrt(squares / (values.shape[0] * values.shape[2]) + norm_eps)


def on_device(tokens, pre_gain, post_gain, gate_weight, up_weight, down_weight):
    layers = gate_weight.shape[0]
    chips = lax.axis_size(CHIP)
    cores = lax.axis_size("core")
    core = lax.axis_index("core")
    place = jnp.stack((core, lax.axis_index("col_2")))

    halves = lax.axis_size("row")
    count = tokens.shape[0] // halves
    gains = copies_of(jnp.concatenate((pre_gain, post_gain), axis=0), "row")
    mixed = tokens.reshape(halves, count, tokens.shape[1]).astype(jnp.float32)
    mixed = exchanged(jnp.concatenate((mixed, gains), axis=1), "row")
    current = mixed[:, :count].astype(jnp.bfloat16)
    gains = 1.0 + mixed[:, count:]

    other_down = lax.ppermute(down_weight, "core", SWAP)
    first, later = packed(gate_weight, up_weight, chips)
    first, other_down = lax.optimization_barrier((first, other_down))
    first = exchanged(first, CHIP)
    later = exchanged(later, CHIP)

    for layer in range(layers):
        values = current.astype(jnp.float32)
        normed = (values * scale_of(values) * gains[:, layer][:, None]).astype(jnp.bfloat16)
        cut = exchanged(slabs(normed, chips, cores), "core")
        cut = cut.reshape(cores * count, -1)
        everything = exchanged(copies_of(cut, CHIP), CHIP).reshape(-1, cut.shape[1])
        weights = first if layer == 0 else later
        mine, theirs = gate_up(everything, weights, first, layer, core, cores)
        got = lax.ppermute(theirs, "core", SWAP)
        sent = down(mine, got, down_weight, other_down, layer, place, chips)
        if layer == 0:
            sent, later = lax.optimization_barrier((sent, later))
        arrived = exchanged(sent, CHIP)
        branch = jnp.sum(arrived.astype(jnp.float32), axis=0).reshape(values.shape)
        post = branch * scale_of(branch) * gains[:, layers + layer][:, None]
        current = (values + post).astype(jnp.bfloat16)
    return exchanged(current, "row").reshape(tokens.shape)


def solution(mesh):
    split = Mesh(
        mesh.devices.reshape(mesh.shape["row"], 4, 4, 2, 2),
        ROW_COL,
    )
    in_specs = (
        P(COL, "row"),
        P(None, "row"),
        P(None, "row"),
        P(None, ROW_COL, None),
        P(None, ROW_COL, None),
        P(None, ROW_COL, None),
    )
    out_specs = P(COL, "row")

    return jax.shard_map(
        on_device, mesh=split, in_specs=in_specs, out_specs=out_specs, check_vma=False
    )
```

```python
import functools

import jax
import jax.numpy as jnp
from jax import lax
from jax.experimental import pallas as pl
from jax.experimental.pallas import tpu as pltpu
from jax.sharding import Mesh
from jax.sharding import PartitionSpec as P

COL = ("col_0", "col_1", "col_2", "core")
ROW_COL = ("row", *COL)
CHIP = ("row", "col_0", "col_1", "col_2")

ORDER = ("col_2", "row", "col_0", "col_1")
SWAP = [(0, 1), (1, 0)]

norm_eps = 1e-06


def pack_kernel(gate_ref, up_ref, first_ref, later_ref):
    rows, layers, lanes = gate_ref.shape
    pairs = first_ref.shape[0] // 2
    width = lanes // pairs
    whole = rows // 8 * 8
    rest = rows - whole
    half = width // 2
    aligned = half // 128 * 128
    odd = half - aligned
    for pair in range(pairs):
        for index, ref in enumerate((gate_ref, up_ref)):
            block = jnp.swapaxes(ref[:, :, pair * width : (pair + 1) * width], 0, 1)
            for side in range(2):
                first = 0 if side == 0 else width - aligned
                extra = aligned if side == 0 else half
                main = slice(index * aligned, (index + 1) * aligned)
                tail = slice(2 * aligned + index * odd, 2 * aligned + (index + 1) * odd)
                place = 2 * pair + side
                for layer in range(layers):
                    out_ref = first_ref if layer == 0 else later_ref
                    start = 0 if layer == 0 else (layer - 1) * whole
                    put = slice(start, start + whole)
                    out_ref[place, put, main] = block[layer, :whole, first : first + aligned]
                    out_ref[place, put, tail] = block[layer, :whole, extra : extra + odd]
                    put = slice(whole + layer * rest, whole + (layer + 1) * rest)
                    first_ref[place, put, main] = block[layer, whole:, first : first + aligned]
                    first_ref[place, put, tail] = block[layer, whole:, extra : extra + odd]


def packed(gate_weight, up_weight, chips):
    layers, rows, hidden = gate_weight.shape
    width = hidden // chips * 2
    whole = rows // 8 * 8
    pairs = 4
    taken = pl.BlockSpec((rows, layers, pairs * width), lambda i: (0, 0, i))
    lengths = (whole + layers * (rows - whole), (layers - 1) * whole)
    return pl.pallas_call(
        pack_kernel,
        grid=(chips // 2 // pairs,),
        in_specs=[taken, taken],
        out_specs=[pl.BlockSpec((2 * pairs, n, width), lambda i: (i, 0, 0)) for n in lengths],
        out_shape=[jax.ShapeDtypeStruct((chips, n, width), gate_weight.dtype) for n in lengths],
        compiler_params=pltpu.CompilerParams(vmem_limit_bytes=59 * 2**20),
        name="pack",
    )(jnp.swapaxes(gate_weight, 0, 1), jnp.swapaxes(up_weight, 0, 1))


def bits(length):
    return length.bit_length() - 1


def one_hot(place, taken):
    return (place == taken).astype(jnp.float32).astype(jnp.bfloat16)


def turned(low, high):
    low_first = lax.broadcasted_iota(jnp.int32, low.shape, 1) < low.shape[1] // 2
    low_turned = pltpu.roll(low, low.shape[1] // 2, 1)
    high_turned = pltpu.roll(high, low.shape[1] // 2, 1)
    return jnp.where(low_first, low, high_turned), jnp.where(low_first, low_turned, high)


def gate_up_kernel(layer, core_ref, normed_ref, *refs):
    weight_ref, rest_ref, weight_end_ref, rest_end_ref = refs[:4]
    own_ref, other_ref, spread_ref = refs[4:]
    chips, whole, _ = weight_ref.shape
    rest = rest_ref.shape[1]
    narrow = normed_ref.shape[1] - chips * whole
    step = pl.program_id(0)

    @pl.when(step == 0)
    def _():
        part = narrow // chips
        taken = lax.broadcasted_iota(jnp.int32, (narrow, chips * rest), 0)
        put = lax.broadcasted_iota(jnp.int32, (narrow, chips * rest), 1)
        place = ((taken >> bits(part)) << bits(rest)) + layer * part + (taken & (part - 1))
        spread_ref[...] = jnp.dot(
            normed_ref[:, chips * whole :],
            one_hot(place, put),
            preferred_element_type=jnp.float32,
        ).astype(jnp.bfloat16)

    def product(main_ref, tail_ref, lanes):
        width = main_ref.shape[2]
        part = jnp.dot(
            normed_ref[:, : chips * whole],
            main_ref[...].reshape(chips * whole, width),
            preferred_element_type=jnp.float32,
        )
        part += jnp.dot(
            spread_ref[...],
            tail_ref[...].reshape(chips * rest, width),
            preferred_element_type=jnp.float32,
        )
        part = part.reshape(chips, -1, width)
        first, second = turned(part[: chips // 2], part[chips // 2 :])
        first = first.reshape(-1, width).astype(own_ref.dtype)
        second = second.reshape(-1, width).astype(own_ref.dtype)

        @pl.when(core_ref[0] == 0)
        def _():
            own_ref[:, lanes] = first
            other_ref[:, lanes] = second

        @pl.when(core_ref[0] != 0)
        def _():
            own_ref[:, lanes] = second
            other_ref[:, lanes] = first

    width = weight_ref.shape[2]
    product(weight_ref, rest_ref, pl.ds(pl.multiple_of(step * width, width), width))

    @pl.when(step == pl.num_programs(0) - 1)
    def _():
        end = weight_end_ref.shape[2]
        product(weight_end_ref, rest_end_ref, slice(own_ref.shape[1] - end, own_ref.shape[1]))


def gate_up(normed, weights, rests, layer, core, cores):
    tokens, depth = normed.shape
    chips, _, width = weights.shape
    layers = 2
    rows = depth // chips
    whole = rows // 8 * 8
    rest = layers * (rows - whole)
    step = 256
    end = width % step
    own = tokens // cores
    kept = pl.BlockSpec((own, width), lambda i: (0, 0))
    return pl.pallas_call(
        functools.partial(gate_up_kernel, layer),
        grid=(width // step,),
        in_specs=[
            pl.BlockSpec(memory_space=pltpu.SMEM),
            pl.BlockSpec((tokens, depth), lambda i: (0, 0)),
            pl.BlockSpec((chips, whole, step), lambda i: (0, 0, i)),
            pl.BlockSpec((chips, rest, step), lambda i: (0, whole // rest, i)),
            pl.BlockSpec((chips, whole, end), lambda i: (0, 0, width // end - 1)),
            pl.BlockSpec((chips, rest, end), lambda i: (0, whole // rest, width // end - 1)),
        ],
        out_specs=[kept, kept],
        out_shape=[jax.ShapeDtypeStruct((own, width), jnp.bfloat16)] * 2,
        scratch_shapes=[pltpu.VMEM((tokens, chips * rest), jnp.bfloat16)],
        compiler_params=pltpu.CompilerParams(vmem_limit_bytes=56 * 2**20),
        name="gate_up",
    )(core.reshape(1), normed, weights, rests, weights, rests)


def down_kernel(place_ref, mine_ref, got_ref, *refs):
    own_low_ref, own_high_ref, other_low_ref, other_high_ref, out_ref = refs[:5]
    hidden_ref, turned_ref, weight_ref = refs[5:]
    _, width = mine_ref.shape
    half = width // 2
    aligned = half // 128 * 128
    stored = half // 2
    chips, put_rows, step = out_ref.shape

    @pl.when(pl.program_id(0) == 0)
    def _():
        summed = mine_ref[...].astype(jnp.float32) + got_ref[...].astype(jnp.float32)
        main = jax.nn.gelu(summed[:, :aligned], approximate=True)
        main = (main * summed[:, aligned : 2 * aligned]).astype(jnp.bfloat16)
        tail = jax.nn.gelu(summed[:, 2 * aligned : half + aligned], approximate=True)
        tail = (tail * summed[:, half + aligned :]).astype(jnp.bfloat16)

        @pl.when(place_ref[1] == 0)
        def _():
            turned_ref[:, :aligned] = main
            turned_ref[:, aligned:] = tail

        @pl.when(place_ref[1] != 0)
        def _():
            turned_ref[:, : half - aligned] = tail
            turned_ref[:, half - aligned :] = main

        @pl.when(place_ref[0] == 0)
        def _():
            hidden_ref[...] = turned_ref[...]

        @pl.when(place_ref[0] != 0)
        def _():
            hidden_ref[:, :stored] = turned_ref[:, stored:]
            hidden_ref[:, stored:] = turned_ref[:, :stored]

    sides = []
    for mine, theirs in ((own_low_ref, other_low_ref), (own_high_ref, other_high_ref)):
        weight_ref[:stored] = mine[0]
        weight_ref[stored:] = theirs[0]
        part = jnp.dot(hidden_ref[...], weight_ref[...], preferred_element_type=jnp.float32)
        sides.append(part.reshape(chips // 2, put_rows, step))
    even, odd = turned(*sides)
    both = jnp.stack((even, odd), axis=1).reshape(chips, put_rows, step)
    out_ref[...] = both.astype(out_ref.dtype)


def down(mine, got, own_down, other_down, layer, place, chips):
    rows, width = mine.shape
    _, stored, model_width = own_down.shape
    step = 768
    steps = model_width // 2 // step
    whole = pl.BlockSpec((rows, width), lambda i: (0, 0))
    low = pl.BlockSpec((1, stored, step), lambda i: (layer, 0, i))
    high = pl.BlockSpec((1, stored, step), lambda i: (layer, 0, steps + i))
    put_rows = 2 * rows // chips
    return pl.pallas_call(
        down_kernel,
        grid=(steps,),
        in_specs=[pl.BlockSpec(memory_space=pltpu.SMEM), whole, whole, low, high, low, high],
        out_specs=pl.BlockSpec((chips, put_rows, step), lambda i: (0, 0, i)),
        out_shape=jax.ShapeDtypeStruct((chips, put_rows, model_width // 2), jnp.bfloat16),
        scratch_shapes=[
            pltpu.VMEM((rows, width // 2), jnp.bfloat16),
            pltpu.VMEM((rows, width // 2), jnp.bfloat16),
            pltpu.VMEM((width // 2, step), jnp.bfloat16),
        ],
        compiler_params=pltpu.CompilerParams(vmem_limit_bytes=48 * 2**20),
        name="down",
    )(place, mine, got, own_down, own_down, other_down, other_down)


def copies_of(value, axes):
    return jnp.broadcast_to(value, (lax.axis_size(axes), *value.shape))


def exchanged(blocks, axes):
    return lax.all_to_all(blocks, axes, split_axis=0, concat_axis=0, tiled=True)


def swapped(blocks, axis):
    index = lax.axis_index(axis)
    own = jnp.where(index == 0, blocks[0], blocks[1])
    got = lax.ppermute(jnp.where(index == 0, blocks[1], blocks[0]), axis, SWAP)
    return jnp.where(index == 0, jnp.stack((own, got)), jnp.stack((got, own)))


def slabs(normed, chips, cores):
    halves, count, model_half = normed.shape
    rows = model_half * halves // (chips * cores)
    whole = rows // 8 * 8
    cut = normed.reshape(halves, count, chips // halves, cores, rows).transpose(3, 1, 0, 2, 4)
    main = cut[..., :whole].reshape(cores, count, chips * whole)
    tail = cut[..., whole:].reshape(cores, count, chips * (rows - whole))
    return jnp.concatenate((main, tail), axis=2)


def scale_of(values):
    squares = jnp.sum(values * values, axis=(0, 2), keepdims=True)
    return lax.rsqrt(squares / (values.shape[0] * values.shape[2]) + norm_eps)


def on_device(tokens, pre_gain, post_gain, gate_weight, up_weight, down_weight):
    layers = gate_weight.shape[0]
    chips = lax.axis_size(CHIP)
    cores = lax.axis_size("core")
    core = lax.axis_index("core")
    place = jnp.stack((core, lax.axis_index("col_2")))

    halves = lax.axis_size("row")
    count = tokens.shape[0] // halves
    current = swapped(tokens.reshape(halves, count, tokens.shape[1]), "row")
    gains = jnp.concatenate((pre_gain, post_gain), axis=0)
    gains = 1.0 + swapped(jnp.stack((gains, gains)), "row")

    other_down = lax.ppermute(down_weight, "core", SWAP)
    first, later = packed(gate_weight, up_weight, chips)
    values = current.astype(jnp.float32)
    normed = (values * scale_of(values) * gains[:, 0][:, None]).astype(jnp.bfloat16)
    cut = swapped(slabs(normed, chips, cores), "core").reshape(cores * count, -1)
    first, other_down, cut = lax.optimization_barrier((first, other_down, cut))
    everything = lax.all_gather(cut, ORDER, axis=0, tiled=True)
    first = exchanged(first, CHIP)
    later = exchanged(later, CHIP)

    for layer in range(layers):
        values = current.astype(jnp.float32)
        if layer > 0:
            normed = (values * scale_of(values) * gains[:, layer][:, None]).astype(jnp.bfloat16)
            cut = swapped(slabs(normed, chips, cores), "core").reshape(cores * count, -1)
            everything = exchanged(copies_of(cut, ORDER), ORDER).reshape(-1, cut.shape[1])
        weights = first if layer == 0 else later
        mine, theirs = gate_up(everything, weights, first, layer, core, cores)
        got = lax.ppermute(theirs, "core", SWAP)
        sent = down(mine, got, down_weight, other_down, layer, place, chips)
        if layer == 0:
            sent, later = lax.optimization_barrier((sent, later))
        arrived = exchanged(sent, CHIP)
        branch = jnp.sum(arrived.astype(jnp.float32), axis=0).reshape(values.shape)
        post = branch * scale_of(branch) * gains[:, layers + layer][:, None]
        current = (values + post).astype(jnp.bfloat16)
    return swapped(current, "row").reshape(tokens.shape)


def solution(mesh):
    split = Mesh(
        mesh.devices.reshape(mesh.shape["row"], 4, 4, 2, 2),
        ROW_COL,
    )
    in_specs = (
        P(COL, "row"),
        P(None, "row"),
        P(None, "row"),
        P(None, ROW_COL, None),
        P(None, ROW_COL, None),
        P(None, ROW_COL, None),
    )
    out_specs = P(COL, "row")

    return jax.shard_map(
        on_device, mesh=split, in_specs=in_specs, out_specs=out_specs, check_vma=False
    )
```

```python
import functools

import jax
import jax.numpy as jnp
from jax import lax
from jax.experimental import pallas as pl
from jax.experimental.pallas import tpu as pltpu
from jax.sharding import Mesh
from jax.sharding import PartitionSpec as P

COL = ("col_0", "col_1", "col_2", "core")
ROW_COL = ("row", *COL)
CHIP = ("row", "col_0", "col_1", "col_2")

ORDER = ("col_2", "row", "col_0", "col_1")
SWAP = [(0, 1), (1, 0)]

norm_eps = 1e-06


def pack_kernel(gate_ref, up_ref, first_ref, later_ref):
    rows, layers, lanes = gate_ref.shape
    pairs = first_ref.shape[0] // 2
    width = lanes // pairs
    whole = rows // 8 * 8
    rest = rows - whole
    half = width // 2
    aligned = half // 128 * 128
    odd = half - aligned
    for pair in range(pairs):
        for index, ref in enumerate((gate_ref, up_ref)):
            block = jnp.swapaxes(ref[:, :, pair * width : (pair + 1) * width], 0, 1)
            for side in range(2):
                first = 0 if side == 0 else width - aligned
                extra = aligned if side == 0 else half
                main = slice(index * aligned, (index + 1) * aligned)
                tail = slice(2 * aligned + index * odd, 2 * aligned + (index + 1) * odd)
                place = 2 * pair + side
                for layer in range(layers):
                    out_ref = first_ref if layer == 0 else later_ref
                    start = 0 if layer == 0 else (layer - 1) * whole
                    put = slice(start, start + whole)
                    out_ref[place, put, main] = block[layer, :whole, first : first + aligned]
                    out_ref[place, put, tail] = block[layer, :whole, extra : extra + odd]
                    put = slice(whole + layer * rest, whole + (layer + 1) * rest)
                    first_ref[place, put, main] = block[layer, whole:, first : first + aligned]
                    first_ref[place, put, tail] = block[layer, whole:, extra : extra + odd]


def packed(gate_weight, up_weight, chips):
    layers, rows, hidden = gate_weight.shape
    width = hidden // chips * 2
    whole = rows // 8 * 8
    pairs = 4
    taken = pl.BlockSpec((rows, layers, pairs * width), lambda i: (0, 0, i))
    lengths = (whole + layers * (rows - whole), (layers - 1) * whole)
    return pl.pallas_call(
        pack_kernel,
        grid=(chips // 2 // pairs,),
        in_specs=[taken, taken],
        out_specs=[pl.BlockSpec((2 * pairs, n, width), lambda i: (i, 0, 0)) for n in lengths],
        out_shape=[jax.ShapeDtypeStruct((chips, n, width), gate_weight.dtype) for n in lengths],
        compiler_params=pltpu.CompilerParams(vmem_limit_bytes=59 * 2**20),
        name="pack",
    )(jnp.swapaxes(gate_weight, 0, 1), jnp.swapaxes(up_weight, 0, 1))


def bits(length):
    return length.bit_length() - 1


def one_hot(place, taken):
    return (place == taken).astype(jnp.float32).astype(jnp.bfloat16)


def turned(low, high):
    low_first = lax.broadcasted_iota(jnp.int32, low.shape, 1) < low.shape[1] // 2
    low_turned = pltpu.roll(low, low.shape[1] // 2, 1)
    high_turned = pltpu.roll(high, low.shape[1] // 2, 1)
    return jnp.where(low_first, low, high_turned), jnp.where(low_first, low_turned, high)


def gate_up_kernel(layer, core_ref, normed_ref, *refs):
    weight_ref, rest_ref, weight_end_ref, rest_end_ref = refs[:4]
    own_ref, other_ref, spread_ref = refs[4:]
    chips, whole, _ = weight_ref.shape
    rest = rest_ref.shape[1]
    narrow = normed_ref.shape[1] - chips * whole
    step = pl.program_id(0)

    @pl.when(step == 0)
    def _():
        part = narrow // chips
        taken = lax.broadcasted_iota(jnp.int32, (narrow, chips * rest), 0)
        put = lax.broadcasted_iota(jnp.int32, (narrow, chips * rest), 1)
        place = ((taken >> bits(part)) << bits(rest)) + layer * part + (taken & (part - 1))
        spread_ref[...] = jnp.dot(
            normed_ref[:, chips * whole :],
            one_hot(place, put),
            preferred_element_type=jnp.float32,
        ).astype(jnp.bfloat16)

    def product(main_ref, tail_ref, lanes):
        width = main_ref.shape[2]
        part = jnp.dot(
            normed_ref[:, : chips * whole],
            main_ref[...].reshape(chips * whole, width),
            preferred_element_type=jnp.float32,
        )
        part += jnp.dot(
            spread_ref[...],
            tail_ref[...].reshape(chips * rest, width),
            preferred_element_type=jnp.float32,
        )
        part = part.reshape(chips, -1, width)
        first, second = turned(part[: chips // 2], part[chips // 2 :])
        first = first.reshape(-1, width).astype(own_ref.dtype)
        second = second.reshape(-1, width).astype(own_ref.dtype)

        @pl.when(core_ref[0] == 0)
        def _():
            own_ref[:, lanes] = first
            other_ref[:, lanes] = second

        @pl.when(core_ref[0] != 0)
        def _():
            own_ref[:, lanes] = second
            other_ref[:, lanes] = first

    width = weight_ref.shape[2]
    product(weight_ref, rest_ref, pl.ds(pl.multiple_of(step * width, width), width))

    @pl.when(step == pl.num_programs(0) - 1)
    def _():
        end = weight_end_ref.shape[2]
        product(weight_end_ref, rest_end_ref, slice(own_ref.shape[1] - end, own_ref.shape[1]))


def gate_up(normed, weights, rests, layer, core, cores):
    tokens, depth = normed.shape
    chips, _, width = weights.shape
    layers = 2
    rows = depth // chips
    whole = rows // 8 * 8
    rest = layers * (rows - whole)
    step = 256
    end = width % step
    own = tokens // cores
    kept = pl.BlockSpec((own, width), lambda i: (0, 0))
    return pl.pallas_call(
        functools.partial(gate_up_kernel, layer),
        grid=(width // step,),
        in_specs=[
            pl.BlockSpec(memory_space=pltpu.SMEM),
            pl.BlockSpec((tokens, depth), lambda i: (0, 0)),
            pl.BlockSpec((chips, whole, step), lambda i: (0, 0, i)),
            pl.BlockSpec((chips, rest, step), lambda i: (0, whole // rest, i)),
            pl.BlockSpec((chips, whole, end), lambda i: (0, 0, width // end - 1)),
            pl.BlockSpec((chips, rest, end), lambda i: (0, whole // rest, width // end - 1)),
        ],
        out_specs=[kept, kept],
        out_shape=[jax.ShapeDtypeStruct((own, width), jnp.bfloat16)] * 2,
        scratch_shapes=[pltpu.VMEM((tokens, chips * rest), jnp.bfloat16)],
        compiler_params=pltpu.CompilerParams(vmem_limit_bytes=56 * 2**20),
        name="gate_up",
    )(core.reshape(1), normed, weights, rests, weights, rests)


def down_kernel(place_ref, mine_ref, got_ref, *refs):
    own_low_ref, own_high_ref, other_low_ref, other_high_ref, out_ref = refs[:5]
    hidden_ref, turned_ref, weight_ref = refs[5:]
    _, width = mine_ref.shape
    half = width // 2
    aligned = half // 128 * 128
    stored = half // 2
    chips, put_rows, step = out_ref.shape

    @pl.when(pl.program_id(0) == 0)
    def _():
        summed = mine_ref[...].astype(jnp.float32) + got_ref[...].astype(jnp.float32)
        main = jax.nn.gelu(summed[:, :aligned], approximate=True)
        main = (main * summed[:, aligned : 2 * aligned]).astype(jnp.bfloat16)
        tail = jax.nn.gelu(summed[:, 2 * aligned : half + aligned], approximate=True)
        tail = (tail * summed[:, half + aligned :]).astype(jnp.bfloat16)

        @pl.when(place_ref[1] == 0)
        def _():
            turned_ref[:, :aligned] = main
            turned_ref[:, aligned:] = tail

        @pl.when(place_ref[1] != 0)
        def _():
            turned_ref[:, : half - aligned] = tail
            turned_ref[:, half - aligned :] = main

        @pl.when(place_ref[0] == 0)
        def _():
            hidden_ref[...] = turned_ref[...]

        @pl.when(place_ref[0] != 0)
        def _():
            hidden_ref[:, :stored] = turned_ref[:, stored:]
            hidden_ref[:, stored:] = turned_ref[:, :stored]

    sides = []
    for mine, theirs in ((own_low_ref, other_low_ref), (own_high_ref, other_high_ref)):
        weight_ref[:stored] = mine[0]
        weight_ref[stored:] = theirs[0]
        part = jnp.dot(hidden_ref[...], weight_ref[...], preferred_element_type=jnp.float32)
        sides.append(part.reshape(chips // 2, put_rows, step))
    even, odd = turned(*sides)
    both = jnp.stack((even, odd), axis=1).reshape(chips, put_rows, step)
    out_ref[...] = both.astype(out_ref.dtype)


def down(mine, got, own_down, other_down, layer, place, chips):
    rows, width = mine.shape
    _, stored, model_width = own_down.shape
    step = 768
    steps = model_width // 2 // step
    whole = pl.BlockSpec((rows, width), lambda i: (0, 0))
    low = pl.BlockSpec((1, stored, step), lambda i: (layer, 0, i))
    high = pl.BlockSpec((1, stored, step), lambda i: (layer, 0, steps + i))
    put_rows = 2 * rows // chips
    return pl.pallas_call(
        down_kernel,
        grid=(steps,),
        in_specs=[pl.BlockSpec(memory_space=pltpu.SMEM), whole, whole, low, high, low, high],
        out_specs=pl.BlockSpec((chips, put_rows, step), lambda i: (0, 0, i)),
        out_shape=jax.ShapeDtypeStruct((chips, put_rows, model_width // 2), jnp.bfloat16),
        scratch_shapes=[
            pltpu.VMEM((rows, width // 2), jnp.bfloat16),
            pltpu.VMEM((rows, width // 2), jnp.bfloat16),
            pltpu.VMEM((width // 2, step), jnp.bfloat16),
        ],
        compiler_params=pltpu.CompilerParams(vmem_limit_bytes=48 * 2**20),
        name="down",
    )(place, mine, got, own_down, own_down, other_down, other_down)


def copies_of(value, axes):
    return jnp.broadcast_to(value, (lax.axis_size(axes), *value.shape))


def exchanged(blocks, axes):
    return lax.all_to_all(blocks, axes, split_axis=0, concat_axis=0, tiled=True)


def swapped(blocks, axis):
    index = lax.axis_index(axis)
    own = jnp.where(index == 0, blocks[0], blocks[1])
    got = lax.ppermute(jnp.where(index == 0, blocks[1], blocks[0]), axis, SWAP)
    return jnp.where(index == 0, jnp.stack((own, got)), jnp.stack((got, own)))


def slabs(normed, chips, cores):
    halves, count, model_half = normed.shape
    rows = model_half * halves // (chips * cores)
    whole = rows // 8 * 8
    cut = normed.reshape(halves, count, chips // halves, cores, rows).transpose(3, 1, 0, 2, 4)
    main = cut[..., :whole].reshape(cores, count, chips * whole)
    tail = cut[..., whole:].reshape(cores, count, chips * (rows - whole))
    return jnp.concatenate((main, tail), axis=2)


def scale_of(values):
    squares = jnp.sum(values * values, axis=(0, 2), keepdims=True)
    return lax.rsqrt(squares / (values.shape[0] * values.shape[2]) + norm_eps)


def on_device(tokens, pre_gain, post_gain, gate_weight, up_weight, down_weight):
    layers = gate_weight.shape[0]
    chips = lax.axis_size(CHIP)
    cores = lax.axis_size("core")
    core = lax.axis_index("core")
    place = jnp.stack((core, lax.axis_index("col_2")))

    halves = lax.axis_size("row")
    count = tokens.shape[0] // halves
    current = swapped(tokens.reshape(halves, count, tokens.shape[1]), "row")
    gains = jnp.concatenate((pre_gain, post_gain), axis=0)
    gains = 1.0 + swapped(jnp.stack((gains, gains)), "row")

    first, later = packed(gate_weight, up_weight, chips)
    values = current.astype(jnp.float32)
    normed = (values * scale_of(values) * gains[:, 0][:, None]).astype(jnp.bfloat16)
    cut = swapped(slabs(normed, chips, cores), "core").reshape(cores * count, -1)
    cut, leaving = lax.optimization_barrier((cut, down_weight))
    other_down = lax.ppermute(leaving, "core", SWAP)
    everything = exchanged(copies_of(cut, ORDER), ORDER).reshape(-1, cut.shape[1])
    first, other_down, everything = lax.optimization_barrier((first, other_down, everything))
    first = exchanged(first, CHIP)
    later = exchanged(later, CHIP)

    for layer in range(layers):
        values = current.astype(jnp.float32)
        if layer > 0:
            normed = (values * scale_of(values) * gains[:, layer][:, None]).astype(jnp.bfloat16)
            cut = swapped(slabs(normed, chips, cores), "core").reshape(cores * count, -1)
            everything = exchanged(copies_of(cut, ORDER), ORDER).reshape(-1, cut.shape[1])
        weights = first if layer == 0 else later
        mine, theirs = gate_up(everything, weights, first, layer, core, cores)
        got = lax.ppermute(theirs, "core", SWAP)
        sent = down(mine, got, down_weight, other_down, layer, place, chips)
        if layer == 0:
            sent, later = lax.optimization_barrier((sent, later))
        arrived = exchanged(sent, CHIP)
        branch = jnp.sum(arrived.astype(jnp.float32), axis=0).reshape(values.shape)
        post = branch * scale_of(branch) * gains[:, layers + layer][:, None]
        current = (values + post).astype(jnp.bfloat16)
    return swapped(current, "row").reshape(tokens.shape)


def solution(mesh):
    split = Mesh(
        mesh.devices.reshape(mesh.shape["row"], 4, 4, 2, 2),
        ROW_COL,
    )
    in_specs = (
        P(COL, "row"),
        P(None, "row"),
        P(None, "row"),
        P(None, ROW_COL, None),
        P(None, ROW_COL, None),
        P(None, ROW_COL, None),
    )
    out_specs = P(COL, "row")

    return jax.shard_map(
        on_device, mesh=split, in_specs=in_specs, out_specs=out_specs, check_vma=False
    )
```

```python
import functools

import jax
import jax.numpy as jnp
from jax import lax
from jax.experimental import pallas as pl
from jax.experimental.pallas import tpu as pltpu
from jax.sharding import Mesh
from jax.sharding import PartitionSpec as P

COL = ("col_0", "col_1", "col_2", "core")
ROW_COL = ("row", *COL)
CHIP = ("row", "col_0", "col_1", "col_2")

ORDER = ("col_2", "row", "col_0", "col_1")
SWAP = [(0, 1), (1, 0)]

norm_eps = 1e-06


def pack_kernel(gate_ref, up_ref, first_ref, later_ref):
    rows, layers, lanes = gate_ref.shape
    pairs = first_ref.shape[0] // 2
    width = lanes // pairs
    whole = rows // 8 * 8
    rest = rows - whole
    half = width // 2
    aligned = half // 128 * 128
    odd = half - aligned
    for pair in range(pairs):
        for index, ref in enumerate((gate_ref, up_ref)):
            block = jnp.swapaxes(ref[:, :, pair * width : (pair + 1) * width], 0, 1)
            for side in range(2):
                first = 0 if side == 0 else width - aligned
                extra = aligned if side == 0 else half
                main = slice(index * aligned, (index + 1) * aligned)
                tail = slice(2 * aligned + index * odd, 2 * aligned + (index + 1) * odd)
                place = 2 * pair + side
                for layer in range(layers):
                    out_ref = first_ref if layer == 0 else later_ref
                    start = 0 if layer == 0 else (layer - 1) * whole
                    put = slice(start, start + whole)
                    out_ref[place, put, main] = block[layer, :whole, first : first + aligned]
                    out_ref[place, put, tail] = block[layer, :whole, extra : extra + odd]
                    put = slice(whole + layer * rest, whole + (layer + 1) * rest)
                    first_ref[place, put, main] = block[layer, whole:, first : first + aligned]
                    first_ref[place, put, tail] = block[layer, whole:, extra : extra + odd]


def packed(gate_weight, up_weight, chips):
    layers, rows, hidden = gate_weight.shape
    width = hidden // chips * 2
    whole = rows // 8 * 8
    pairs = 4
    taken = pl.BlockSpec((rows, layers, pairs * width), lambda i: (0, 0, i))
    lengths = (whole + layers * (rows - whole), (layers - 1) * whole)
    return pl.pallas_call(
        pack_kernel,
        grid=(chips // 2 // pairs,),
        in_specs=[taken, taken],
        out_specs=[pl.BlockSpec((2 * pairs, n, width), lambda i: (i, 0, 0)) for n in lengths],
        out_shape=[jax.ShapeDtypeStruct((chips, n, width), gate_weight.dtype) for n in lengths],
        compiler_params=pltpu.CompilerParams(vmem_limit_bytes=59 * 2**20),
        name="pack",
    )(jnp.swapaxes(gate_weight, 0, 1), jnp.swapaxes(up_weight, 0, 1))


def bits(length):
    return length.bit_length() - 1


def one_hot(place, taken):
    return (place == taken).astype(jnp.float32).astype(jnp.bfloat16)


def turned(low, high):
    low_first = lax.broadcasted_iota(jnp.int32, low.shape, 1) < low.shape[1] // 2
    low_turned = pltpu.roll(low, low.shape[1] // 2, 1)
    high_turned = pltpu.roll(high, low.shape[1] // 2, 1)
    return jnp.where(low_first, low, high_turned), jnp.where(low_first, low_turned, high)


def gate_up_kernel(layer, core_ref, normed_ref, *refs):
    weight_ref, rest_ref, weight_end_ref, rest_end_ref = refs[:4]
    own_ref, other_ref, spread_ref = refs[4:]
    chips, whole, _ = weight_ref.shape
    rest = rest_ref.shape[1]
    narrow = normed_ref.shape[1] - chips * whole
    step = pl.program_id(0)

    @pl.when(step == 0)
    def _():
        part = narrow // chips
        taken = lax.broadcasted_iota(jnp.int32, (narrow, chips * rest), 0)
        put = lax.broadcasted_iota(jnp.int32, (narrow, chips * rest), 1)
        place = ((taken >> bits(part)) << bits(rest)) + layer * part + (taken & (part - 1))
        spread_ref[...] = jnp.dot(
            normed_ref[:, chips * whole :],
            one_hot(place, put),
            preferred_element_type=jnp.float32,
        ).astype(jnp.bfloat16)

    def product(main_ref, tail_ref, lanes):
        width = main_ref.shape[2]
        part = jnp.dot(
            normed_ref[:, : chips * whole],
            main_ref[...].reshape(chips * whole, width),
            preferred_element_type=jnp.float32,
        )
        part += jnp.dot(
            spread_ref[...],
            tail_ref[...].reshape(chips * rest, width),
            preferred_element_type=jnp.float32,
        )
        part = part.reshape(chips, -1, width)
        first, second = turned(part[: chips // 2], part[chips // 2 :])
        first = first.reshape(-1, width).astype(own_ref.dtype)
        second = second.reshape(-1, width).astype(own_ref.dtype)

        @pl.when(core_ref[0] == 0)
        def _():
            own_ref[:, lanes] = first
            other_ref[:, lanes] = second

        @pl.when(core_ref[0] != 0)
        def _():
            own_ref[:, lanes] = second
            other_ref[:, lanes] = first

    width = weight_ref.shape[2]
    product(weight_ref, rest_ref, pl.ds(pl.multiple_of(step * width, width), width))

    @pl.when(step == pl.num_programs(0) - 1)
    def _():
        end = weight_end_ref.shape[2]
        product(weight_end_ref, rest_end_ref, slice(own_ref.shape[1] - end, own_ref.shape[1]))


def gate_up(normed, weights, rests, layer, core, cores):
    tokens, depth = normed.shape
    chips, _, width = weights.shape
    layers = 2
    rows = depth // chips
    whole = rows // 8 * 8
    rest = layers * (rows - whole)
    step = 256
    end = width % step
    own = tokens // cores
    kept = pl.BlockSpec((own, width), lambda i: (0, 0))
    return pl.pallas_call(
        functools.partial(gate_up_kernel, layer),
        grid=(width // step,),
        in_specs=[
            pl.BlockSpec(memory_space=pltpu.SMEM),
            pl.BlockSpec((tokens, depth), lambda i: (0, 0)),
            pl.BlockSpec((chips, whole, step), lambda i: (0, 0, i)),
            pl.BlockSpec((chips, rest, step), lambda i: (0, whole // rest, i)),
            pl.BlockSpec((chips, whole, end), lambda i: (0, 0, width // end - 1)),
            pl.BlockSpec((chips, rest, end), lambda i: (0, whole // rest, width // end - 1)),
        ],
        out_specs=[kept, kept],
        out_shape=[jax.ShapeDtypeStruct((own, width), jnp.bfloat16)] * 2,
        scratch_shapes=[pltpu.VMEM((tokens, chips * rest), jnp.bfloat16)],
        compiler_params=pltpu.CompilerParams(vmem_limit_bytes=56 * 2**20),
        name="gate_up",
    )(core.reshape(1), normed, weights, rests, weights, rests)


def part_kernel(core_ref, whole_ref, own_ref, other_ref):
    chips = whole_ref.shape[0] // 8
    width = whole_ref.shape[1]
    part = whole_ref[...].astype(jnp.float32).reshape(chips, 8, width)
    first, second = turned(part[: chips // 2], part[chips // 2 :])
    first = first.reshape(-1, width).astype(own_ref.dtype)
    second = second.reshape(-1, width).astype(own_ref.dtype)

    @pl.when(core_ref[0] == 0)
    def _():
        own_ref[...] = first
        other_ref[...] = second

    @pl.when(core_ref[0] != 0)
    def _():
        own_ref[...] = second
        other_ref[...] = first


def parted(whole, core, cores):
    tokens, width = whole.shape
    own = tokens // cores
    return pl.pallas_call(
        part_kernel,
        in_specs=[pl.BlockSpec(memory_space=pltpu.SMEM), pl.BlockSpec(memory_space=pltpu.VMEM)],
        out_specs=[pl.BlockSpec(memory_space=pltpu.VMEM)] * 2,
        out_shape=[jax.ShapeDtypeStruct((own, width), jnp.bfloat16)] * 2,
        compiler_params=pltpu.CompilerParams(vmem_limit_bytes=20 * 2**20),
        name="parted",
    )(core.reshape(1), whole)


def down_kernel(place_ref, mine_ref, got_ref, *refs):
    own_low_ref, own_high_ref, other_low_ref, other_high_ref, out_ref = refs[:5]
    hidden_ref, turned_ref, weight_ref = refs[5:]
    _, width = mine_ref.shape
    half = width // 2
    aligned = half // 128 * 128
    stored = half // 2
    chips, put_rows, step = out_ref.shape

    @pl.when(pl.program_id(0) == 0)
    def _():
        summed = mine_ref[...].astype(jnp.float32) + got_ref[...].astype(jnp.float32)
        main = jax.nn.gelu(summed[:, :aligned], approximate=True)
        main = (main * summed[:, aligned : 2 * aligned]).astype(jnp.bfloat16)
        tail = jax.nn.gelu(summed[:, 2 * aligned : half + aligned], approximate=True)
        tail = (tail * summed[:, half + aligned :]).astype(jnp.bfloat16)

        @pl.when(place_ref[1] == 0)
        def _():
            turned_ref[:, :aligned] = main
            turned_ref[:, aligned:] = tail

        @pl.when(place_ref[1] != 0)
        def _():
            turned_ref[:, : half - aligned] = tail
            turned_ref[:, half - aligned :] = main

        @pl.when(place_ref[0] == 0)
        def _():
            hidden_ref[...] = turned_ref[...]

        @pl.when(place_ref[0] != 0)
        def _():
            hidden_ref[:, :stored] = turned_ref[:, stored:]
            hidden_ref[:, stored:] = turned_ref[:, :stored]

    sides = []
    for mine, theirs in ((own_low_ref, other_low_ref), (own_high_ref, other_high_ref)):
        weight_ref[:stored] = mine[0]
        weight_ref[stored:] = theirs[0]
        part = jnp.dot(hidden_ref[...], weight_ref[...], preferred_element_type=jnp.float32)
        sides.append(part.reshape(chips // 2, put_rows, step))
    even, odd = turned(*sides)
    both = jnp.stack((even, odd), axis=1).reshape(chips, put_rows, step)
    out_ref[...] = both.astype(out_ref.dtype)


def down(mine, got, own_down, other_down, layer, place, chips):
    rows, width = mine.shape
    _, stored, model_width = own_down.shape
    step = 768
    steps = model_width // 2 // step
    whole = pl.BlockSpec((rows, width), lambda i: (0, 0))
    low = pl.BlockSpec((1, stored, step), lambda i: (layer, 0, i))
    high = pl.BlockSpec((1, stored, step), lambda i: (layer, 0, steps + i))
    put_rows = 2 * rows // chips
    return pl.pallas_call(
        down_kernel,
        grid=(steps,),
        in_specs=[pl.BlockSpec(memory_space=pltpu.SMEM), whole, whole, low, high, low, high],
        out_specs=pl.BlockSpec((chips, put_rows, step), lambda i: (0, 0, i)),
        out_shape=jax.ShapeDtypeStruct((chips, put_rows, model_width // 2), jnp.bfloat16),
        scratch_shapes=[
            pltpu.VMEM((rows, width // 2), jnp.bfloat16),
            pltpu.VMEM((rows, width // 2), jnp.bfloat16),
            pltpu.VMEM((width // 2, step), jnp.bfloat16),
        ],
        compiler_params=pltpu.CompilerParams(vmem_limit_bytes=48 * 2**20),
        name="down",
    )(place, mine, got, own_down, own_down, other_down, other_down)


def copies_of(value, axes):
    return jnp.broadcast_to(value, (lax.axis_size(axes), *value.shape))


def exchanged(blocks, axes):
    return lax.all_to_all(blocks, axes, split_axis=0, concat_axis=0, tiled=True)


def swapped(blocks, axis):
    index = lax.axis_index(axis)
    own = jnp.where(index == 0, blocks[0], blocks[1])
    got = lax.ppermute(jnp.where(index == 0, blocks[1], blocks[0]), axis, SWAP)
    return jnp.where(index == 0, jnp.stack((own, got)), jnp.stack((got, own)))


def slabs(normed, chips, cores):
    halves, count, model_half = normed.shape
    rows = model_half * halves // (chips * cores)
    whole = rows // 8 * 8
    cut = normed.reshape(halves, count, chips // halves, cores, rows).transpose(3, 1, 0, 2, 4)
    main = cut[..., :whole].reshape(cores, count, chips * whole)
    tail = cut[..., whole:].reshape(cores, count, chips * (rows - whole))
    return jnp.concatenate((main, tail), axis=2)


def scale_of(values):
    squares = jnp.sum(values * values, axis=(0, 2), keepdims=True)
    return lax.rsqrt(squares / (values.shape[0] * values.shape[2]) + norm_eps)


def on_device(tokens, pre_gain, post_gain, gate_weight, up_weight, down_weight):
    layers = gate_weight.shape[0]
    chips = lax.axis_size(CHIP)
    cores = lax.axis_size("core")
    core = lax.axis_index("core")
    place = jnp.stack((core, lax.axis_index("col_2")))

    halves = lax.axis_size("row")
    count = tokens.shape[0] // halves
    current = swapped(tokens.reshape(halves, count, tokens.shape[1]), "row")
    gains = jnp.concatenate((pre_gain, post_gain), axis=0)
    gains = 1.0 + swapped(jnp.stack((gains, gains)), "row")

    first, later = packed(gate_weight, up_weight, chips)
    values = current.astype(jnp.float32)
    normed = (values * scale_of(values) * gains[:, 0][:, None]).astype(jnp.bfloat16)
    cut = swapped(slabs(normed, chips, cores), "core").reshape(cores * count, -1)
    cut, leaving = lax.optimization_barrier((cut, down_weight))
    other_down = lax.ppermute(leaving, "core", SWAP)
    everything = exchanged(copies_of(cut, ORDER), ORDER).reshape(-1, cut.shape[1])
    first, other_down, everything = lax.optimization_barrier((first, other_down, everything))
    first = exchanged(first, CHIP)
    later = exchanged(later, CHIP)

    for layer in range(layers):
        values = current.astype(jnp.float32)
        if layer > 0:
            normed = (values * scale_of(values) * gains[:, layer][:, None]).astype(jnp.bfloat16)
            cut = swapped(slabs(normed, chips, cores), "core").reshape(cores * count, -1)
            everything = exchanged(copies_of(cut, ORDER), ORDER).reshape(-1, cut.shape[1])
        if layer == 0:
            mine, theirs = gate_up(everything, first, first, layer, core, cores)
        else:
            whole = jnp.dot(everything, joined, preferred_element_type=jnp.float32)
            mine, theirs = parted(whole.astype(jnp.bfloat16), core, cores)
        got = lax.ppermute(theirs, "core", SWAP)
        sent = down(mine, got, down_weight, other_down, layer, place, chips)
        if layer == 0:
            sent, later = lax.optimization_barrier((sent, later))
            rest = (first.shape[1] - later.shape[1]) // layers
            tails = first[:, first.shape[1] - rest :].reshape(-1, first.shape[2])
            joined = jnp.concatenate((later.reshape(-1, later.shape[2]), tails), axis=0)
        arrived = exchanged(sent, CHIP)
        branch = jnp.sum(arrived.astype(jnp.float32), axis=0).reshape(values.shape)
        post = branch * scale_of(branch) * gains[:, layers + layer][:, None]
        current = (values + post).astype(jnp.bfloat16)
    return swapped(current, "row").reshape(tokens.shape)


def solution(mesh):
    split = Mesh(
        mesh.devices.reshape(mesh.shape["row"], 4, 4, 2, 2),
        ROW_COL,
    )
    in_specs = (
        P(COL, "row"),
        P(None, "row"),
        P(None, "row"),
        P(None, ROW_COL, None),
        P(None, ROW_COL, None),
        P(None, ROW_COL, None),
    )
    out_specs = P(COL, "row")

    return jax.shard_map(
        on_device, mesh=split, in_specs=in_specs, out_specs=out_specs, check_vma=False
    )
```

```python
import functools

import jax
import jax.numpy as jnp
from jax import lax
from jax.experimental import pallas as pl
from jax.experimental.pallas import tpu as pltpu
from jax.sharding import Mesh
from jax.sharding import PartitionSpec as P

COL = ("col_0", "col_1", "col_2", "core")
ROW_COL = ("row", *COL)
CHIP = ("row", "col_0", "col_1", "col_2")

ORDER = ("col_2", "row", "col_0", "col_1")
SWAP = [(0, 1), (1, 0)]

norm_eps = 1e-06


def pack_kernel(gate_ref, up_ref, first_ref, later_ref):
    rows, layers, lanes = gate_ref.shape
    pairs = first_ref.shape[0] // 2
    width = lanes // pairs
    whole = rows // 8 * 8
    rest = rows - whole
    half = width // 2
    aligned = half // 128 * 128
    odd = half - aligned
    for pair in range(pairs):
        for index, ref in enumerate((gate_ref, up_ref)):
            block = jnp.swapaxes(ref[:, :, pair * width : (pair + 1) * width], 0, 1)
            for side in range(2):
                first = 0 if side == 0 else width - aligned
                extra = aligned if side == 0 else half
                main = slice(index * aligned, (index + 1) * aligned)
                tail = slice(2 * aligned + index * odd, 2 * aligned + (index + 1) * odd)
                place = 2 * pair + side
                for layer in range(layers):
                    out_ref = first_ref if layer == 0 else later_ref
                    start = 0 if layer == 0 else (layer - 1) * whole
                    put = slice(start, start + whole)
                    out_ref[place, put, main] = block[layer, :whole, first : first + aligned]
                    out_ref[place, put, tail] = block[layer, :whole, extra : extra + odd]
                    put = slice(whole + layer * rest, whole + (layer + 1) * rest)
                    first_ref[place, put, main] = block[layer, whole:, first : first + aligned]
                    first_ref[place, put, tail] = block[layer, whole:, extra : extra + odd]


def packed(gate_weight, up_weight, chips, spare):
    layers, rows, hidden = gate_weight.shape
    width = hidden // chips * 2
    whole = rows // 8 * 8
    pairs = 4
    taken = pl.BlockSpec((rows, layers, pairs * width), lambda i: (0, 0, i))
    lengths = (whole + layers * (rows - whole), (layers - 1) * whole)
    room = (lengths[0] + spare, lengths[1])
    return pl.pallas_call(
        pack_kernel,
        grid=(chips // 2 // pairs,),
        in_specs=[taken, taken],
        out_specs=[pl.BlockSpec((2 * pairs, n, width), lambda i: (i, 0, 0)) for n in lengths],
        out_shape=[jax.ShapeDtypeStruct((chips, n, width), gate_weight.dtype) for n in room],
        compiler_params=pltpu.CompilerParams(vmem_limit_bytes=59 * 2**20),
        name="pack",
    )(jnp.swapaxes(gate_weight, 0, 1), jnp.swapaxes(up_weight, 0, 1))


def bits(length):
    return length.bit_length() - 1


def one_hot(place, taken):
    return (place == taken).astype(jnp.float32).astype(jnp.bfloat16)


def board_kernel(cut_ref, held_ref, out_ref):
    del held_ref
    out_ref[...] = jnp.broadcast_to(cut_ref[...][None], out_ref.shape)


def boarded(held, cut):
    chips, rows, width = held.shape
    count, depth = cut.shape
    parts = depth // width
    return pl.pallas_call(
        board_kernel,
        grid=(parts,),
        in_specs=[
            pl.BlockSpec((count, width), lambda i: (0, i)),
            pl.BlockSpec(memory_space=pl.ANY),
        ],
        out_specs=pl.BlockSpec((chips, count, width), lambda i: (0, rows // count - parts + i, 0)),
        out_shape=jax.ShapeDtypeStruct(held.shape, held.dtype),
        input_output_aliases={1: 0},
        compiler_params=pltpu.CompilerParams(vmem_limit_bytes=59 * 2**20),
        name="board",
    )(cut, held)


def turned(low, high):
    low_first = lax.broadcasted_iota(jnp.int32, low.shape, 1) < low.shape[1] // 2
    low_turned = pltpu.roll(low, low.shape[1] // 2, 1)
    high_turned = pltpu.roll(high, low.shape[1] // 2, 1)
    return jnp.where(low_first, low, high_turned), jnp.where(low_first, low_turned, high)


def gate_up_kernel(layer, pieces, core_ref, *refs):
    normed_refs, refs = refs[:pieces], refs[pieces:]
    weight_ref, rest_ref, weight_end_ref, rest_end_ref = refs[:4]
    own_ref, other_ref, spread_ref = refs[4:]
    chips, whole, _ = weight_ref.shape
    rest = rest_ref.shape[1]
    lanes_each = normed_refs[0].shape[-1]
    narrow = pieces * lanes_each - chips * whole
    held = [ref[...].reshape(-1, lanes_each) for ref in normed_refs]
    step = pl.program_id(0)

    @pl.when(step == 0)
    def _():
        part = narrow // chips
        taken = lax.broadcasted_iota(jnp.int32, (narrow, chips * rest), 0)
        put = lax.broadcasted_iota(jnp.int32, (narrow, chips * rest), 1)
        place = ((taken >> bits(part)) << bits(rest)) + layer * part + (taken & (part - 1))
        spread_ref[...] = jnp.dot(
            held[-1][:, lanes_each - narrow :],
            one_hot(place, put),
            preferred_element_type=jnp.float32,
        ).astype(jnp.bfloat16)

    def product(main_ref, tail_ref, lanes):
        width = main_ref.shape[2]
        part = jnp.dot(
            spread_ref[...],
            tail_ref[...].reshape(chips * rest, width),
            preferred_element_type=jnp.float32,
        )
        main = main_ref[...].reshape(chips * whole, width)
        for piece in range(pieces):
            start = piece * lanes_each
            stop = min(start + lanes_each, chips * whole)
            part += jnp.dot(
                held[piece][:, : stop - start],
                main[start:stop],
                preferred_element_type=jnp.float32,
            )
        if pieces == 1:
            part = part.reshape(chips, -1, width)
            first, second = turned(part[: chips // 2], part[chips // 2 :])
        else:
            part = part.reshape(chips // 2, 2, -1, width)
            first, second = turned(part[:, 0], part[:, 1])
        first = first.reshape(-1, width).astype(own_ref.dtype)
        second = second.reshape(-1, width).astype(own_ref.dtype)

        @pl.when(core_ref[0] == 0)
        def _():
            own_ref[:, lanes] = first
            other_ref[:, lanes] = second

        @pl.when(core_ref[0] != 0)
        def _():
            own_ref[:, lanes] = second
            other_ref[:, lanes] = first

    width = weight_ref.shape[2]
    product(weight_ref, rest_ref, pl.ds(pl.multiple_of(step * width, width), width))

    @pl.when(step == pl.num_programs(0) - 1)
    def _():
        end = weight_end_ref.shape[2]
        product(weight_end_ref, rest_end_ref, slice(own_ref.shape[1] - end, own_ref.shape[1]))


def gate_up(normed, weights, rests, layer, core, cores):
    chips, _, width = weights.shape
    layers = 2
    if normed is None:
        count = 4 * cores
        tokens, pieces = chips * count, 2
        depth = pieces * width
        base = rests.shape[1] // count - pieces
        lhs = [rests] * pieces
        lhs_specs = [
            pl.BlockSpec((chips, count, width), lambda i, piece=piece: (0, base + piece, 0))
            for piece in range(pieces)
        ]
    else:
        tokens, depth = normed.shape
        pieces, lhs = 1, [normed]
        lhs_specs = [pl.BlockSpec((tokens, depth), lambda i: (0, 0))]
    rows = depth // chips
    whole = rows // 8 * 8
    rest = layers * (rows - whole)
    step = 256
    end = width % step
    own = tokens // cores
    kept = pl.BlockSpec((own, width), lambda i: (0, 0))
    return pl.pallas_call(
        functools.partial(gate_up_kernel, layer, pieces),
        grid=(width // step,),
        in_specs=[
            pl.BlockSpec(memory_space=pltpu.SMEM),
            *lhs_specs,
            pl.BlockSpec((chips, whole, step), lambda i: (0, 0, i)),
            pl.BlockSpec((chips, rest, step), lambda i: (0, whole // rest, i)),
            pl.BlockSpec((chips, whole, end), lambda i: (0, 0, width // end - 1)),
            pl.BlockSpec((chips, rest, end), lambda i: (0, whole // rest, width // end - 1)),
        ],
        out_specs=[kept, kept],
        out_shape=[jax.ShapeDtypeStruct((own, width), jnp.bfloat16)] * 2,
        scratch_shapes=[pltpu.VMEM((tokens, chips * rest), jnp.bfloat16)],
        compiler_params=pltpu.CompilerParams(vmem_limit_bytes=56 * 2**20),
        name="gate_up",
    )(core.reshape(1), *lhs, weights, rests, weights, rests)


def down_kernel(place_ref, mine_ref, got_ref, *refs):
    own_low_ref, own_high_ref, other_low_ref, other_high_ref, out_ref = refs[:5]
    hidden_ref, turned_ref, weight_ref = refs[5:]
    _, width = mine_ref.shape
    half = width // 2
    aligned = half // 128 * 128
    stored = half // 2
    chips, put_rows, step = out_ref.shape

    @pl.when(pl.program_id(0) == 0)
    def _():
        summed = mine_ref[...].astype(jnp.float32) + got_ref[...].astype(jnp.float32)
        main = jax.nn.gelu(summed[:, :aligned], approximate=True)
        main = (main * summed[:, aligned : 2 * aligned]).astype(jnp.bfloat16)
        tail = jax.nn.gelu(summed[:, 2 * aligned : half + aligned], approximate=True)
        tail = (tail * summed[:, half + aligned :]).astype(jnp.bfloat16)

        @pl.when(place_ref[1] == 0)
        def _():
            turned_ref[:, :aligned] = main
            turned_ref[:, aligned:] = tail

        @pl.when(place_ref[1] != 0)
        def _():
            turned_ref[:, : half - aligned] = tail
            turned_ref[:, half - aligned :] = main

        @pl.when(place_ref[0] == 0)
        def _():
            hidden_ref[...] = turned_ref[...]

        @pl.when(place_ref[0] != 0)
        def _():
            hidden_ref[:, :stored] = turned_ref[:, stored:]
            hidden_ref[:, stored:] = turned_ref[:, :stored]

    sides = []
    for mine, theirs in ((own_low_ref, other_low_ref), (own_high_ref, other_high_ref)):
        weight_ref[:stored] = mine[0]
        weight_ref[stored:] = theirs[0]
        part = jnp.dot(hidden_ref[...], weight_ref[...], preferred_element_type=jnp.float32)
        sides.append(part.reshape(chips // 2, put_rows, step))
    even, odd = turned(*sides)
    both = jnp.stack((even, odd), axis=1).reshape(chips, put_rows, step)
    out_ref[...] = both.astype(out_ref.dtype)


def down(mine, got, own_down, other_down, layer, place, chips):
    rows, width = mine.shape
    _, stored, model_width = own_down.shape
    step = 768
    steps = model_width // 2 // step
    whole = pl.BlockSpec((rows, width), lambda i: (0, 0))
    low = pl.BlockSpec((1, stored, step), lambda i: (layer, 0, i))
    high = pl.BlockSpec((1, stored, step), lambda i: (layer, 0, steps + i))
    put_rows = 2 * rows // chips
    return pl.pallas_call(
        down_kernel,
        grid=(steps,),
        in_specs=[pl.BlockSpec(memory_space=pltpu.SMEM), whole, whole, low, high, low, high],
        out_specs=pl.BlockSpec((chips, put_rows, step), lambda i: (0, 0, i)),
        out_shape=jax.ShapeDtypeStruct((chips, put_rows, model_width // 2), jnp.bfloat16),
        scratch_shapes=[
            pltpu.VMEM((rows, width // 2), jnp.bfloat16),
            pltpu.VMEM((rows, width // 2), jnp.bfloat16),
            pltpu.VMEM((width // 2, step), jnp.bfloat16),
        ],
        compiler_params=pltpu.CompilerParams(vmem_limit_bytes=48 * 2**20),
        name="down",
    )(place, mine, got, own_down, own_down, other_down, other_down)


def copies_of(value, axes):
    return jnp.broadcast_to(value, (lax.axis_size(axes), *value.shape))


def exchanged(blocks, axes):
    return lax.all_to_all(blocks, axes, split_axis=0, concat_axis=0, tiled=True)


def swapped(blocks, axis):
    index = lax.axis_index(axis)
    own = jnp.where(index == 0, blocks[0], blocks[1])
    got = lax.ppermute(jnp.where(index == 0, blocks[1], blocks[0]), axis, SWAP)
    return jnp.where(index == 0, jnp.stack((own, got)), jnp.stack((got, own)))


def slabs(normed, chips, cores):
    halves, count, model_half = normed.shape
    rows = model_half * halves // (chips * cores)
    whole = rows // 8 * 8
    cut = normed.reshape(halves, count, chips // halves, cores, rows).transpose(3, 1, 0, 2, 4)
    main = cut[..., :whole].reshape(cores, count, chips * whole)
    tail = cut[..., whole:].reshape(cores, count, chips * (rows - whole))
    return jnp.concatenate((main, tail), axis=2)


def scale_of(values):
    squares = jnp.sum(values * values, axis=(0, 2), keepdims=True)
    return lax.rsqrt(squares / (values.shape[0] * values.shape[2]) + norm_eps)


def on_device(tokens, pre_gain, post_gain, gate_weight, up_weight, down_weight):
    layers = gate_weight.shape[0]
    chips = lax.axis_size(CHIP)
    cores = lax.axis_size("core")
    core = lax.axis_index("core")
    place = jnp.stack((core, lax.axis_index("col_2")))

    halves = lax.axis_size("row")
    count = tokens.shape[0] // halves
    current = swapped(tokens.reshape(halves, count, tokens.shape[1]), "row")
    gains = jnp.concatenate((pre_gain, post_gain), axis=0)
    gains = 1.0 + swapped(jnp.stack((gains, gains)), "row")

    spare = 4 * cores * 2
    first, later = packed(gate_weight, up_weight, chips, spare)
    values = current.astype(jnp.float32)
    normed = (values * scale_of(values) * gains[:, 0][:, None]).astype(jnp.bfloat16)
    cut = swapped(slabs(normed, chips, cores), "core").reshape(cores * count, -1)
    cut, leaving = lax.optimization_barrier((cut, down_weight))
    other_down = lax.ppermute(leaving, "core", SWAP)
    everything = None
    first, other_down = lax.optimization_barrier((boarded(first, cut), other_down))
    first = exchanged(first, CHIP)
    later = exchanged(later, CHIP)

    for layer in range(layers):
        values = current.astype(jnp.float32)
        if layer > 0:
            normed = (values * scale_of(values) * gains[:, layer][:, None]).astype(jnp.bfloat16)
            cut = swapped(slabs(normed, chips, cores), "core").reshape(cores * count, -1)
            everything = exchanged(copies_of(cut, ORDER), ORDER).reshape(-1, cut.shape[1])
        weights = first if layer == 0 else later
        mine, theirs = gate_up(everything, weights, first, layer, core, cores)
        got = lax.ppermute(theirs, "core", SWAP)
        sent = down(mine, got, down_weight, other_down, layer, place, chips)
        if layer == 0:
            sent, later = lax.optimization_barrier((sent, later))
        arrived = exchanged(sent, CHIP)
        branch = jnp.sum(arrived.astype(jnp.float32), axis=0).reshape(values.shape)
        post = branch * scale_of(branch) * gains[:, layers + layer][:, None]
        current = (values + post).astype(jnp.bfloat16)
    return swapped(current, "row").reshape(tokens.shape)


def solution(mesh):
    split = Mesh(
        mesh.devices.reshape(mesh.shape["row"], 4, 4, 2, 2),
        ROW_COL,
    )
    in_specs = (
        P(COL, "row"),
        P(None, "row"),
        P(None, "row"),
        P(None, ROW_COL, None),
        P(None, ROW_COL, None),
        P(None, ROW_COL, None),
    )
    out_specs = P(COL, "row")

    return jax.shard_map(
        on_device, mesh=split, in_specs=in_specs, out_specs=out_specs, check_vma=False
    )
```

```python
import functools

import jax
import jax.numpy as jnp
from jax import lax
from jax.experimental import pallas as pl
from jax.experimental.pallas import tpu as pltpu
from jax.sharding import Mesh
from jax.sharding import PartitionSpec as P

COL = ("col_0", "col_1", "col_2", "core")
ROW_COL = ("row", *COL)
CHIP = ("row", "col_0", "col_1", "col_2")

ORDER = ("col_2", "row", "col_0", "col_1")
SWAP = [(0, 1), (1, 0)]

norm_eps = 1e-06


def pack_kernel(early, gate_ref, up_ref, out_ref):
    rows, layers, lanes = gate_ref.shape
    pairs = out_ref.shape[0] // 2
    width = lanes // pairs
    whole = rows // 8 * 8
    rest = rows - whole
    half = width // 2
    aligned = half // 128 * 128
    odd = half - aligned
    for pair in range(pairs):
        for index, ref in enumerate((gate_ref, up_ref)):
            block = jnp.swapaxes(ref[:, :, pair * width : (pair + 1) * width], 0, 1)
            for side in range(2):
                first = 0 if side == 0 else width - aligned
                extra = aligned if side == 0 else half
                main = slice(index * aligned, (index + 1) * aligned)
                tail = slice(2 * aligned + index * odd, 2 * aligned + (index + 1) * odd)
                place = 2 * pair + side
                for layer in range(layers):
                    if early == (layer == 0):
                        start = max(layer - 1, 0) * whole
                        put = slice(start, start + whole)
                        out_ref[place, put, main] = block[layer, :whole, first : first + aligned]
                        out_ref[place, put, tail] = block[layer, :whole, extra : extra + odd]
                    if early:
                        put = slice(whole + layer * rest, whole + (layer + 1) * rest)
                        out_ref[place, put, main] = block[layer, whole:, first : first + aligned]
                        out_ref[place, put, tail] = block[layer, whole:, extra : extra + odd]


def packed(gate_weight, up_weight, chips, early, spare):
    layers, rows, hidden = gate_weight.shape
    width = hidden // chips * 2
    whole = rows // 8 * 8
    pairs = 4
    taken = pl.BlockSpec((rows, layers, pairs * width), lambda i: (0, 0, i))
    length = whole + layers * (rows - whole) if early else (layers - 1) * whole
    return pl.pallas_call(
        functools.partial(pack_kernel, early),
        grid=(chips // 2 // pairs,),
        in_specs=[taken, taken],
        out_specs=pl.BlockSpec((2 * pairs, length, width), lambda i: (i, 0, 0)),
        out_shape=jax.ShapeDtypeStruct((chips, length + spare, width), gate_weight.dtype),
        compiler_params=pltpu.CompilerParams(vmem_limit_bytes=59 * 2**20),
        name="pack_early" if early else "pack_late",
    )(jnp.swapaxes(gate_weight, 0, 1), jnp.swapaxes(up_weight, 0, 1))


def bits(length):
    return length.bit_length() - 1


def one_hot(place, taken):
    return (place == taken).astype(jnp.float32).astype(jnp.bfloat16)


def board_kernel(cut_ref, held_ref, out_ref):
    del held_ref
    out_ref[...] = jnp.broadcast_to(cut_ref[...][None], out_ref.shape)


def boarded(held, cut):
    chips, rows, width = held.shape
    count, depth = cut.shape
    parts = depth // width
    return pl.pallas_call(
        board_kernel,
        grid=(parts,),
        in_specs=[
            pl.BlockSpec((count, width), lambda i: (0, i)),
            pl.BlockSpec(memory_space=pl.ANY),
        ],
        out_specs=pl.BlockSpec((chips, count, width), lambda i: (0, rows // count - parts + i, 0)),
        out_shape=jax.ShapeDtypeStruct(held.shape, held.dtype),
        input_output_aliases={1: 0},
        compiler_params=pltpu.CompilerParams(vmem_limit_bytes=59 * 2**20),
        name="board",
    )(cut, held)


def turned(low, high):
    low_first = lax.broadcasted_iota(jnp.int32, low.shape, 1) < low.shape[1] // 2
    low_turned = pltpu.roll(low, low.shape[1] // 2, 1)
    high_turned = pltpu.roll(high, low.shape[1] // 2, 1)
    return jnp.where(low_first, low, high_turned), jnp.where(low_first, low_turned, high)


def gate_up_kernel(layer, pieces, core_ref, *refs):
    normed_refs, refs = refs[:pieces], refs[pieces:]
    weight_ref, rest_ref, weight_end_ref, rest_end_ref = refs[:4]
    own_ref, other_ref, spread_ref = refs[4:]
    chips, whole, _ = weight_ref.shape
    rest = rest_ref.shape[1]
    lanes_each = normed_refs[0].shape[-1]
    narrow = pieces * lanes_each - chips * whole
    held = [ref[...].reshape(-1, lanes_each) for ref in normed_refs]
    step = pl.program_id(0)

    @pl.when(step == 0)
    def _():
        part = narrow // chips
        taken = lax.broadcasted_iota(jnp.int32, (narrow, chips * rest), 0)
        put = lax.broadcasted_iota(jnp.int32, (narrow, chips * rest), 1)
        place = ((taken >> bits(part)) << bits(rest)) + layer * part + (taken & (part - 1))
        spread_ref[...] = jnp.dot(
            held[-1][:, lanes_each - narrow :],
            one_hot(place, put),
            preferred_element_type=jnp.float32,
        ).astype(jnp.bfloat16)

    def product(main_ref, tail_ref, lanes):
        width = main_ref.shape[2]
        part = jnp.dot(
            spread_ref[...],
            tail_ref[...].reshape(chips * rest, width),
            preferred_element_type=jnp.float32,
        )
        main = main_ref[...].reshape(chips * whole, width)
        for piece in range(pieces):
            start = piece * lanes_each
            stop = min(start + lanes_each, chips * whole)
            part += jnp.dot(
                held[piece][:, : stop - start],
                main[start:stop],
                preferred_element_type=jnp.float32,
            )
        if pieces == 1:
            part = part.reshape(chips, -1, width)
            first, second = turned(part[: chips // 2], part[chips // 2 :])
        else:
            part = part.reshape(chips // 2, 2, -1, width)
            first, second = turned(part[:, 0], part[:, 1])
        first = first.reshape(-1, width).astype(own_ref.dtype)
        second = second.reshape(-1, width).astype(own_ref.dtype)

        @pl.when(core_ref[0] == 0)
        def _():
            own_ref[:, lanes] = first
            other_ref[:, lanes] = second

        @pl.when(core_ref[0] != 0)
        def _():
            own_ref[:, lanes] = second
            other_ref[:, lanes] = first

    width = weight_ref.shape[2]
    product(weight_ref, rest_ref, pl.ds(pl.multiple_of(step * width, width), width))

    @pl.when(step == pl.num_programs(0) - 1)
    def _():
        end = weight_end_ref.shape[2]
        product(weight_end_ref, rest_end_ref, slice(own_ref.shape[1] - end, own_ref.shape[1]))


def gate_up(normed, weights, rests, layer, core, cores):
    chips, _, width = weights.shape
    layers = 2
    if normed is None:
        count = 4 * cores
        tokens, pieces = chips * count, 2
        depth = pieces * width
        base = rests.shape[1] // count - pieces
        lhs = [rests] * pieces
        lhs_specs = [
            pl.BlockSpec((chips, count, width), lambda i, piece=piece: (0, base + piece, 0))
            for piece in range(pieces)
        ]
    else:
        tokens, depth = normed.shape
        pieces, lhs = 1, [normed]
        lhs_specs = [pl.BlockSpec((tokens, depth), lambda i: (0, 0))]
    rows = depth // chips
    whole = rows // 8 * 8
    rest = layers * (rows - whole)
    step = 256
    end = width % step
    own = tokens // cores
    kept = pl.BlockSpec((own, width), lambda i: (0, 0))
    return pl.pallas_call(
        functools.partial(gate_up_kernel, layer, pieces),
        grid=(width // step,),
        in_specs=[
            pl.BlockSpec(memory_space=pltpu.SMEM),
            *lhs_specs,
            pl.BlockSpec((chips, whole, step), lambda i: (0, 0, i)),
            pl.BlockSpec((chips, rest, step), lambda i: (0, whole // rest, i)),
            pl.BlockSpec((chips, whole, end), lambda i: (0, 0, width // end - 1)),
            pl.BlockSpec((chips, rest, end), lambda i: (0, whole // rest, width // end - 1)),
        ],
        out_specs=[kept, kept],
        out_shape=[jax.ShapeDtypeStruct((own, width), jnp.bfloat16)] * 2,
        scratch_shapes=[pltpu.VMEM((tokens, chips * rest), jnp.bfloat16)],
        compiler_params=pltpu.CompilerParams(vmem_limit_bytes=56 * 2**20),
        name="gate_up",
    )(core.reshape(1), *lhs, weights, rests, weights, rests)


def part_kernel(core_ref, whole_ref, own_ref, other_ref):
    chips = whole_ref.shape[0] // 8
    width = whole_ref.shape[1]
    part = whole_ref[...].astype(jnp.float32).reshape(chips, 8, width)
    first, second = turned(part[: chips // 2], part[chips // 2 :])
    first = first.reshape(-1, width).astype(own_ref.dtype)
    second = second.reshape(-1, width).astype(own_ref.dtype)

    @pl.when(core_ref[0] == 0)
    def _():
        own_ref[...] = first
        other_ref[...] = second

    @pl.when(core_ref[0] != 0)
    def _():
        own_ref[...] = second
        other_ref[...] = first


def parted(whole, core, cores):
    tokens, width = whole.shape
    own = tokens // cores
    return pl.pallas_call(
        part_kernel,
        in_specs=[pl.BlockSpec(memory_space=pltpu.SMEM), pl.BlockSpec(memory_space=pltpu.VMEM)],
        out_specs=[pl.BlockSpec(memory_space=pltpu.VMEM)] * 2,
        out_shape=[jax.ShapeDtypeStruct((own, width), jnp.bfloat16)] * 2,
        compiler_params=pltpu.CompilerParams(vmem_limit_bytes=20 * 2**20),
        name="parted",
    )(core.reshape(1), whole)


def down_kernel(place_ref, mine_ref, got_ref, *refs):
    own_low_ref, own_high_ref, other_low_ref, other_high_ref, out_ref = refs[:5]
    hidden_ref, turned_ref, weight_ref = refs[5:]
    _, width = mine_ref.shape
    half = width // 2
    aligned = half // 128 * 128
    stored = half // 2
    chips, put_rows, step = out_ref.shape

    @pl.when(pl.program_id(0) == 0)
    def _():
        summed = mine_ref[...].astype(jnp.float32) + got_ref[...].astype(jnp.float32)
        main = jax.nn.gelu(summed[:, :aligned], approximate=True)
        main = (main * summed[:, aligned : 2 * aligned]).astype(jnp.bfloat16)
        tail = jax.nn.gelu(summed[:, 2 * aligned : half + aligned], approximate=True)
        tail = (tail * summed[:, half + aligned :]).astype(jnp.bfloat16)

        @pl.when(place_ref[1] == 0)
        def _():
            turned_ref[:, :aligned] = main
            turned_ref[:, aligned:] = tail

        @pl.when(place_ref[1] != 0)
        def _():
            turned_ref[:, : half - aligned] = tail
            turned_ref[:, half - aligned :] = main

        @pl.when(place_ref[0] == 0)
        def _():
            hidden_ref[...] = turned_ref[...]

        @pl.when(place_ref[0] != 0)
        def _():
            hidden_ref[:, :stored] = turned_ref[:, stored:]
            hidden_ref[:, stored:] = turned_ref[:, :stored]

    sides = []
    for mine, theirs in ((own_low_ref, other_low_ref), (own_high_ref, other_high_ref)):
        weight_ref[:stored] = mine[0]
        weight_ref[stored:] = theirs[0]
        part = jnp.dot(hidden_ref[...], weight_ref[...], preferred_element_type=jnp.float32)
        sides.append(part.reshape(chips // 2, put_rows, step))
    even, odd = turned(*sides)
    both = jnp.stack((even, odd), axis=1).reshape(chips, put_rows, step)
    out_ref[...] = both.astype(out_ref.dtype)


def down(mine, got, own_down, other_down, layer, place, chips):
    rows, width = mine.shape
    _, stored, model_width = own_down.shape
    step = 768
    steps = model_width // 2 // step
    whole = pl.BlockSpec((rows, width), lambda i: (0, 0))
    low = pl.BlockSpec((1, stored, step), lambda i: (layer, 0, i))
    high = pl.BlockSpec((1, stored, step), lambda i: (layer, 0, steps + i))
    put_rows = 2 * rows // chips
    return pl.pallas_call(
        down_kernel,
        grid=(steps,),
        in_specs=[pl.BlockSpec(memory_space=pltpu.SMEM), whole, whole, low, high, low, high],
        out_specs=pl.BlockSpec((chips, put_rows, step), lambda i: (0, 0, i)),
        out_shape=jax.ShapeDtypeStruct((chips, put_rows, model_width // 2), jnp.bfloat16),
        scratch_shapes=[
            pltpu.VMEM((rows, width // 2), jnp.bfloat16),
            pltpu.VMEM((rows, width // 2), jnp.bfloat16),
            pltpu.VMEM((width // 2, step), jnp.bfloat16),
        ],
        compiler_params=pltpu.CompilerParams(vmem_limit_bytes=48 * 2**20),
        name="down",
    )(place, mine, got, own_down, own_down, other_down, other_down)


def copies_of(value, axes):
    return jnp.broadcast_to(value, (lax.axis_size(axes), *value.shape))


def exchanged(blocks, axes):
    return lax.all_to_all(blocks, axes, split_axis=0, concat_axis=0, tiled=True)


def swapped(blocks, axis):
    index = lax.axis_index(axis)
    own = jnp.where(index == 0, blocks[0], blocks[1])
    got = lax.ppermute(jnp.where(index == 0, blocks[1], blocks[0]), axis, SWAP)
    return jnp.where(index == 0, jnp.stack((own, got)), jnp.stack((got, own)))


def slabs(normed, chips, cores):
    halves, count, model_half = normed.shape
    rows = model_half * halves // (chips * cores)
    whole = rows // 8 * 8
    cut = normed.reshape(halves, count, chips // halves, cores, rows).transpose(3, 1, 0, 2, 4)
    main = cut[..., :whole].reshape(cores, count, chips * whole)
    tail = cut[..., whole:].reshape(cores, count, chips * (rows - whole))
    return jnp.concatenate((main, tail), axis=2)


def scale_of(values):
    squares = jnp.sum(values * values, axis=(0, 2), keepdims=True)
    return lax.rsqrt(squares / (values.shape[0] * values.shape[2]) + norm_eps)


def on_device(tokens, pre_gain, post_gain, gate_weight, up_weight, down_weight):
    layers = gate_weight.shape[0]
    chips = lax.axis_size(CHIP)
    cores = lax.axis_size("core")
    core = lax.axis_index("core")
    place = jnp.stack((core, lax.axis_index("col_2")))

    halves = lax.axis_size("row")
    count = tokens.shape[0] // halves
    current = swapped(tokens.reshape(halves, count, tokens.shape[1]), "row")
    gains = jnp.concatenate((pre_gain, post_gain), axis=0)
    gains = 1.0 + swapped(jnp.stack((gains, gains)), "row")

    spare = 4 * cores * 2
    first = packed(gate_weight, up_weight, chips, True, spare)
    later = packed(gate_weight, up_weight, chips, False, 0)
    values = current.astype(jnp.float32)
    normed = (values * scale_of(values) * gains[:, 0][:, None]).astype(jnp.bfloat16)
    cut = swapped(slabs(normed, chips, cores), "core").reshape(cores * count, -1)
    cut, leaving = lax.optimization_barrier((cut, down_weight))
    other_down = lax.ppermute(leaving, "core", SWAP)
    everything = None
    first, other_down = lax.optimization_barrier((boarded(first, cut), other_down))
    first = exchanged(first, CHIP)
    later = exchanged(later, CHIP)

    for layer in range(layers):
        values = current.astype(jnp.float32)
        if layer > 0:
            normed = (values * scale_of(values) * gains[:, layer][:, None]).astype(jnp.bfloat16)
            cut = swapped(slabs(normed, chips, cores), "core").reshape(cores * count, -1)
            everything = exchanged(copies_of(cut, ORDER), ORDER).reshape(-1, cut.shape[1])
        if layer == 0:
            mine, theirs = gate_up(everything, first, first, layer, core, cores)
        else:
            whole = jnp.dot(everything, joined, preferred_element_type=jnp.float32)
            mine, theirs = parted(whole.astype(jnp.bfloat16), core, cores)
        got = lax.ppermute(theirs, "core", SWAP)
        sent = down(mine, got, down_weight, other_down, layer, place, chips)
        if layer == 0:
            rows = gate_weight.shape[1]
            tails = first[:, rows : rows + rows - later.shape[1]].reshape(-1, first.shape[2])
            sent, later, tails = lax.optimization_barrier((sent, later, tails))
            joined = jnp.concatenate((later.reshape(-1, later.shape[2]), tails), axis=0)
        arrived = exchanged(sent, CHIP)
        branch = jnp.sum(arrived.astype(jnp.float32), axis=0).reshape(values.shape)
        post = branch * scale_of(branch) * gains[:, layers + layer][:, None]
        current = (values + post).astype(jnp.bfloat16)
    return swapped(current, "row").reshape(tokens.shape)


def solution(mesh):
    split = Mesh(
        mesh.devices.reshape(mesh.shape["row"], 4, 4, 2, 2),
        ROW_COL,
    )
    in_specs = (
        P(COL, "row"),
        P(None, "row"),
        P(None, "row"),
        P(None, ROW_COL, None),
        P(None, ROW_COL, None),
        P(None, ROW_COL, None),
    )
    out_specs = P(COL, "row")

    return jax.shard_map(
        on_device, mesh=split, in_specs=in_specs, out_specs=out_specs, check_vma=False
    )
```

```python
import functools

import jax
import jax.numpy as jnp
from jax import lax
from jax.experimental import pallas as pl
from jax.experimental.pallas import tpu as pltpu
from jax.sharding import Mesh
from jax.sharding import PartitionSpec as P

COL = ("col_0", "col_1", "col_2", "core")
ROW_COL = ("row", *COL)
CHIP = ("row", "col_0", "col_1", "col_2")

ORDER = ("col_2", "row", "col_0", "col_1")
SWAP = [(0, 1), (1, 0)]

norm_eps = 1e-06


def pack_kernel(gate_ref, up_ref, first_ref, later_ref):
    rows, layers, lanes = gate_ref.shape
    pairs = first_ref.shape[0] // 2
    width = lanes // pairs
    whole = rows // 8 * 8
    rest = rows - whole
    half = width // 2
    aligned = half // 128 * 128
    odd = half - aligned
    for pair in range(pairs):
        for index, ref in enumerate((gate_ref, up_ref)):
            block = jnp.swapaxes(ref[:, :, pair * width : (pair + 1) * width], 0, 1)
            for side in range(2):
                first = 0 if side == 0 else width - aligned
                extra = aligned if side == 0 else half
                main = slice(index * aligned, (index + 1) * aligned)
                tail = slice(2 * aligned + index * odd, 2 * aligned + (index + 1) * odd)
                place = 2 * pair + side
                for layer in range(layers):
                    out_ref = first_ref if layer == 0 else later_ref
                    start = 0 if layer == 0 else (layer - 1) * whole
                    put = slice(start, start + whole)
                    out_ref[place, put, main] = block[layer, :whole, first : first + aligned]
                    out_ref[place, put, tail] = block[layer, :whole, extra : extra + odd]
                    put = slice(whole + layer * rest, whole + (layer + 1) * rest)
                    first_ref[place, put, main] = block[layer, whole:, first : first + aligned]
                    first_ref[place, put, tail] = block[layer, whole:, extra : extra + odd]


def packed(gate_weight, up_weight, chips):
    layers, rows, hidden = gate_weight.shape
    width = hidden // chips * 2
    whole = rows // 8 * 8
    pairs = 4
    taken = pl.BlockSpec((rows, layers, pairs * width), lambda i: (0, 0, i))
    lengths = (whole + layers * (rows - whole), (layers - 1) * whole)
    return pl.pallas_call(
        pack_kernel,
        grid=(chips // 2 // pairs,),
        in_specs=[taken, taken],
        out_specs=[pl.BlockSpec((2 * pairs, n, width), lambda i: (i, 0, 0)) for n in lengths],
        out_shape=[jax.ShapeDtypeStruct((chips, n, width), gate_weight.dtype) for n in lengths],
        compiler_params=pltpu.CompilerParams(vmem_limit_bytes=59 * 2**20),
        name="pack",
    )(jnp.swapaxes(gate_weight, 0, 1), jnp.swapaxes(up_weight, 0, 1))


def bits(length):
    return length.bit_length() - 1


def one_hot(place, taken):
    return (place == taken).astype(jnp.float32).astype(jnp.bfloat16)


def turned(low, high):
    low_first = lax.broadcasted_iota(jnp.int32, low.shape, 1) < low.shape[1] // 2
    low_turned = pltpu.roll(low, low.shape[1] // 2, 1)
    high_turned = pltpu.roll(high, low.shape[1] // 2, 1)
    return jnp.where(low_first, low, high_turned), jnp.where(low_first, low_turned, high)


def gate_up_kernel(layer, core_ref, normed_ref, *refs):
    weight_ref, rest_ref, weight_end_ref, rest_end_ref = refs[:4]
    own_ref, other_ref, spread_ref = refs[4:]
    chips, whole, _ = weight_ref.shape
    rest = rest_ref.shape[1]
    narrow = normed_ref.shape[1] - chips * whole
    step = pl.program_id(0)

    @pl.when(step == 0)
    def _():
        part = narrow // chips
        taken = lax.broadcasted_iota(jnp.int32, (narrow, chips * rest), 0)
        put = lax.broadcasted_iota(jnp.int32, (narrow, chips * rest), 1)
        place = ((taken >> bits(part)) << bits(rest)) + layer * part + (taken & (part - 1))
        spread_ref[...] = jnp.dot(
            normed_ref[:, chips * whole :],
            one_hot(place, put),
            preferred_element_type=jnp.float32,
        ).astype(jnp.bfloat16)

    def product(main_ref, tail_ref, lanes):
        width = main_ref.shape[2]
        part = jnp.dot(
            normed_ref[:, : chips * whole],
            main_ref[...].reshape(chips * whole, width),
            preferred_element_type=jnp.float32,
        )
        part += jnp.dot(
            spread_ref[...],
            tail_ref[...].reshape(chips * rest, width),
            preferred_element_type=jnp.float32,
        )
        part = part.reshape(chips, -1, width)
        first, second = turned(part[: chips // 2], part[chips // 2 :])
        first = first.reshape(-1, width).astype(own_ref.dtype)
        second = second.reshape(-1, width).astype(own_ref.dtype)

        @pl.when(core_ref[0] == 0)
        def _():
            own_ref[:, lanes] = first
            other_ref[:, lanes] = second

        @pl.when(core_ref[0] != 0)
        def _():
            own_ref[:, lanes] = second
            other_ref[:, lanes] = first

    width = weight_ref.shape[2]
    product(weight_ref, rest_ref, pl.ds(pl.multiple_of(step * width, width), width))

    @pl.when(step == pl.num_programs(0) - 1)
    def _():
        end = weight_end_ref.shape[2]
        product(weight_end_ref, rest_end_ref, slice(own_ref.shape[1] - end, own_ref.shape[1]))


def gate_up(normed, weights, rests, layer, core, cores):
    tokens, depth = normed.shape
    chips, _, width = weights.shape
    layers = 2
    rows = depth // chips
    whole = rows // 8 * 8
    rest = layers * (rows - whole)
    step = 256
    end = width % step
    own = tokens // cores
    kept = pl.BlockSpec((own, width), lambda i: (0, 0))
    return pl.pallas_call(
        functools.partial(gate_up_kernel, layer),
        grid=(width // step,),
        in_specs=[
            pl.BlockSpec(memory_space=pltpu.SMEM),
            pl.BlockSpec((tokens, depth), lambda i: (0, 0)),
            pl.BlockSpec((chips, whole, step), lambda i: (0, 0, i)),
            pl.BlockSpec((chips, rest, step), lambda i: (0, whole // rest, i)),
            pl.BlockSpec((chips, whole, end), lambda i: (0, 0, width // end - 1)),
            pl.BlockSpec((chips, rest, end), lambda i: (0, whole // rest, width // end - 1)),
        ],
        out_specs=[kept, kept],
        out_shape=[jax.ShapeDtypeStruct((own, width), jnp.bfloat16)] * 2,
        scratch_shapes=[pltpu.VMEM((tokens, chips * rest), jnp.bfloat16)],
        compiler_params=pltpu.CompilerParams(vmem_limit_bytes=56 * 2**20),
        name="gate_up",
    )(core.reshape(1), normed, weights, rests, weights, rests)


def part_kernel(core_ref, whole_ref, own_ref, other_ref):
    chips = whole_ref.shape[0] // 8
    width = whole_ref.shape[1]
    part = whole_ref[...].astype(jnp.float32).reshape(chips, 8, width)
    first, second = turned(part[: chips // 2], part[chips // 2 :])
    first = first.reshape(-1, width).astype(own_ref.dtype)
    second = second.reshape(-1, width).astype(own_ref.dtype)

    @pl.when(core_ref[0] == 0)
    def _():
        own_ref[...] = first
        other_ref[...] = second

    @pl.when(core_ref[0] != 0)
    def _():
        own_ref[...] = second
        other_ref[...] = first


def parted(whole, core, cores):
    tokens, width = whole.shape
    own = tokens // cores
    return pl.pallas_call(
        part_kernel,
        in_specs=[pl.BlockSpec(memory_space=pltpu.SMEM), pl.BlockSpec(memory_space=pltpu.VMEM)],
        out_specs=[pl.BlockSpec(memory_space=pltpu.VMEM)] * 2,
        out_shape=[jax.ShapeDtypeStruct((own, width), jnp.bfloat16)] * 2,
        compiler_params=pltpu.CompilerParams(vmem_limit_bytes=20 * 2**20),
        name="parted",
    )(core.reshape(1), whole)


def down_kernel(place_ref, mine_ref, got_ref, *refs):
    own_low_ref, own_high_ref, other_low_ref, other_high_ref, out_ref = refs[:5]
    hidden_ref, turned_ref, weight_ref = refs[5:]
    _, width = mine_ref.shape
    half = width // 2
    aligned = half // 128 * 128
    stored = half // 2
    chips, put_rows, step = out_ref.shape

    @pl.when(pl.program_id(0) == 0)
    def _():
        summed = mine_ref[...].astype(jnp.float32) + got_ref[...].astype(jnp.float32)
        main = jax.nn.gelu(summed[:, :aligned], approximate=True)
        main = (main * summed[:, aligned : 2 * aligned]).astype(jnp.bfloat16)
        tail = jax.nn.gelu(summed[:, 2 * aligned : half + aligned], approximate=True)
        tail = (tail * summed[:, half + aligned :]).astype(jnp.bfloat16)

        @pl.when(place_ref[1] == 0)
        def _():
            turned_ref[:, :aligned] = main
            turned_ref[:, aligned:] = tail

        @pl.when(place_ref[1] != 0)
        def _():
            turned_ref[:, : half - aligned] = tail
            turned_ref[:, half - aligned :] = main

        @pl.when(place_ref[0] == 0)
        def _():
            hidden_ref[...] = turned_ref[...]

        @pl.when(place_ref[0] != 0)
        def _():
            hidden_ref[:, :stored] = turned_ref[:, stored:]
            hidden_ref[:, stored:] = turned_ref[:, :stored]

    sides = []
    for mine, theirs in ((own_low_ref, other_low_ref), (own_high_ref, other_high_ref)):
        weight_ref[:stored] = mine[0]
        weight_ref[stored:] = theirs[0]
        part = jnp.dot(hidden_ref[...], weight_ref[...], preferred_element_type=jnp.float32)
        sides.append(part.reshape(chips // 2, put_rows, step))
    even, odd = turned(*sides)
    both = jnp.stack((even, odd), axis=1).reshape(chips, put_rows, step)
    out_ref[...] = both.astype(out_ref.dtype)


def down(mine, got, own_down, other_down, layer, place, chips):
    rows, width = mine.shape
    _, stored, model_width = own_down.shape
    step = 1152
    steps = model_width // 2 // step
    whole = pl.BlockSpec((rows, width), lambda i: (0, 0))
    low = pl.BlockSpec((1, stored, step), lambda i: (layer, 0, i))
    high = pl.BlockSpec((1, stored, step), lambda i: (layer, 0, steps + i))
    put_rows = 2 * rows // chips
    return pl.pallas_call(
        down_kernel,
        grid=(steps,),
        in_specs=[pl.BlockSpec(memory_space=pltpu.SMEM), whole, whole, low, high, low, high],
        out_specs=pl.BlockSpec((chips, put_rows, step), lambda i: (0, 0, i)),
        out_shape=jax.ShapeDtypeStruct((chips, put_rows, model_width // 2), jnp.bfloat16),
        scratch_shapes=[
            pltpu.VMEM((rows, width // 2), jnp.bfloat16),
            pltpu.VMEM((rows, width // 2), jnp.bfloat16),
            pltpu.VMEM((width // 2, step), jnp.bfloat16),
        ],
        compiler_params=pltpu.CompilerParams(vmem_limit_bytes=48 * 2**20),
        name="down",
    )(place, mine, got, own_down, own_down, other_down, other_down)


def copies_of(value, axes):
    return jnp.broadcast_to(value, (lax.axis_size(axes), *value.shape))


def exchanged(blocks, axes):
    return lax.all_to_all(blocks, axes, split_axis=0, concat_axis=0, tiled=True)


def swapped(blocks, axis):
    index = lax.axis_index(axis)
    own = jnp.where(index == 0, blocks[0], blocks[1])
    got = lax.ppermute(jnp.where(index == 0, blocks[1], blocks[0]), axis, SWAP)
    return jnp.where(index == 0, jnp.stack((own, got)), jnp.stack((got, own)))


def slabs(normed, chips, cores):
    halves, count, model_half = normed.shape
    rows = model_half * halves // (chips * cores)
    whole = rows // 8 * 8
    cut = normed.reshape(halves, count, chips // halves, cores, rows).transpose(3, 1, 0, 2, 4)
    main = cut[..., :whole].reshape(cores, count, chips * whole)
    tail = cut[..., whole:].reshape(cores, count, chips * (rows - whole))
    return jnp.concatenate((main, tail), axis=2)


def scale_of(values):
    squares = jnp.sum(values * values, axis=(0, 2), keepdims=True)
    return lax.rsqrt(squares / (values.shape[0] * values.shape[2]) + norm_eps)


def on_device(tokens, pre_gain, post_gain, gate_weight, up_weight, down_weight):
    layers = gate_weight.shape[0]
    chips = lax.axis_size(CHIP)
    cores = lax.axis_size("core")
    core = lax.axis_index("core")
    place = jnp.stack((core, lax.axis_index("col_2")))

    halves = lax.axis_size("row")
    count = tokens.shape[0] // halves
    current = swapped(tokens.reshape(halves, count, tokens.shape[1]), "row")
    gains = jnp.concatenate((pre_gain, post_gain), axis=0)
    gains = 1.0 + swapped(jnp.stack((gains, gains)), "row")

    first, later = packed(gate_weight, up_weight, chips)
    values = current.astype(jnp.float32)
    normed = (values * scale_of(values) * gains[:, 0][:, None]).astype(jnp.bfloat16)
    cut = swapped(slabs(normed, chips, cores), "core").reshape(cores * count, -1)
    cut, leaving = lax.optimization_barrier((cut, down_weight))
    other_down = lax.ppermute(leaving, "core", SWAP)
    everything = exchanged(copies_of(cut, ORDER), ORDER).reshape(-1, cut.shape[1])
    first, other_down, everything = lax.optimization_barrier((first, other_down, everything))
    first = exchanged(first, CHIP)
    later = exchanged(later, CHIP)

    for layer in range(layers):
        values = current.astype(jnp.float32)
        if layer > 0:
            normed = (values * scale_of(values) * gains[:, layer][:, None]).astype(jnp.bfloat16)
            cut = swapped(slabs(normed, chips, cores), "core").reshape(cores * count, -1)
            everything = exchanged(copies_of(cut, ORDER), ORDER).reshape(-1, cut.shape[1])
        if layer == 0:
            mine, theirs = gate_up(everything, first, first, layer, core, cores)
        else:
            whole = jnp.dot(everything, joined, preferred_element_type=jnp.float32)
            mine, theirs = parted(whole.astype(jnp.bfloat16), core, cores)
        got = lax.ppermute(theirs, "core", SWAP)
        sent = down(mine, got, down_weight, other_down, layer, place, chips)
        if layer == 0:
            rows = gate_weight.shape[1]
            tails = first[:, rows : rows + rows - later.shape[1]].reshape(-1, first.shape[2])
            sent, later, tails = lax.optimization_barrier((sent, later, tails))
            joined = jnp.concatenate((later.reshape(-1, later.shape[2]), tails), axis=0)
        arrived = exchanged(sent, CHIP)
        branch = jnp.sum(arrived.astype(jnp.float32), axis=0).reshape(values.shape)
        post = branch * scale_of(branch) * gains[:, layers + layer][:, None]
        current = (values + post).astype(jnp.bfloat16)
    return swapped(current, "row").reshape(tokens.shape)


def solution(mesh):
    split = Mesh(
        mesh.devices.reshape(mesh.shape["row"], 4, 4, 2, 2),
        ROW_COL,
    )
    in_specs = (
        P(COL, "row"),
        P(None, "row"),
        P(None, "row"),
        P(None, ROW_COL, None),
        P(None, ROW_COL, None),
        P(None, ROW_COL, None),
    )
    out_specs = P(COL, "row")

    return jax.shard_map(
        on_device, mesh=split, in_specs=in_specs, out_specs=out_specs, check_vma=False
    )
```
